128 devices in a mesh: sub: 32 (over x, z, core), grp: 4 (over y).
Axes of the slice: x: 4, y: 4, z: 4, core: 2. Of those that a mesh axis runs over, the one named last changes fastest.
Arguments:
- solution: float32 [128, 128, 2048], P(('sub', 'grp')), may hold values from -6 to 6
- residual: float32 [128, 128, 2048], P(('sub', 'grp'))
- direction: float32 [128, 128, 2048], P(('sub', 'grp'))
- residual_product: float32 [128], replicated, may hold values from 262144 to 5242880
- neighbor_slots: int32 [128, 4], P(('sub', 'grp')), may hold values from 0 to 3, each once within a row
- coupling: bfloat16 [128, 96, 256, 128], P(('sub', 'grp')), may hold values from -0.375 to 0.375
- dirichlet_factor: bfloat16 [128, 96, 128, 128], P(('sub', 'grp')), may hold values from -0.5 to 0.5
- face_block: bfloat16 [128, 32, 128, 128], P(('sub', 'grp')), as said below
- neumann_factor: bfloat16 [128, 32, 128, 128], P(('sub', 'grp')), may hold values from -0.5 to 0.5
- primal_block: int32 [128, 128], P(('sub', 'grp')), may hold values from 0 to 31
- primal_basis: bfloat16 [128, 128, 128], P(('sub', 'grp')), may hold values from -1.5 to 1.5
- coarse_matrix: float32 [128, 9, 128, 128], P(('sub', 'grp')), may hold values from -0.17677669 to 0.17677669
- coarse_block_inverse: float32 [128, 128, 128], P(('sub', 'grp')), may hold values from -0.5 to 0.5
- coarse_pattern: int32 [128, 9], P(('sub', 'grp')), may hold values from 0 to 127, as said below
Outputs:
- new_solution: float32 [128, 128, 2048], P(('sub', 'grp'))
- new_residual: float32 [128, 128, 2048], P(('sub', 'grp'))
- new_direction: float32 [128, 128, 2048], P(('sub', 'grp'))
- new_product: float32 [128], replicated
The draws below stay inside these ranges and needn't reach their ends.
Inputs may be any that keep to these rules, and one draw needn't show every extreme that they name: `neighbor_slots`: each row orders the four local face slots: entry d is the slot of the face toward direction d (sub lower, sub upper, grp lower, grp upper). `coarse_pattern`: row t names 9 different subdomains, the first of them t itself; subdomain s lies on the device of index s along sub+grp, and every entry lies within 2 positions of row t along sub, cyclically. `face_block`: each block is symmetric with every eigenvalue at least 0.5.
All inputs are finite; a program needn't handle non-finite values.
Results may differ from the reference program's by a relative error of at most 0.0003.
Values sent between devices are 32-bit elements; how exact they have to be, the bound alone decides.
A program may use at most 128 MiB of HBM per device.

```python
import math
import jax
import jax.numpy as jnp
from jax import lax

LOAD_CASES = 128
FACE_SIZE = 1024
BLOCK_SIZE = 128
PRIMALS = 128
PATTERN_BLOCKS = 9
REACH_SUBS = 2
FACE_BLOCKS = 32
INNER_BLOCKS = 96
SUBDOMAINS = 128
N_SUB = 32
N_GRP = 4


def ramped_field(key, salt):
    full_shape = (SUBDOMAINS, LOAD_CASES, 2 * FACE_SIZE)
    base_key = jax.random.fold_in(key, salt)
    column = jnp.exp(jax.random.uniform(jax.random.fold_in(base_key, 1), (1, 1, 2 * FACE_SIZE), jnp.float32, math.log(0.3), math.log(3.0)))
    across = jnp.exp(jax.random.uniform(jax.random.fold_in(base_key, 2), (1, LOAD_CASES, 1), jnp.float32, math.log(0.6), math.log(2.0)))
    position = jnp.arange(SUBDOMAINS, dtype=jnp.float32) / (SUBDOMAINS - 1)
    values = jax.random.normal(jax.random.fold_in(base_key, 3), full_shape, jnp.float32)
    ramp_scale = jnp.exp(math.log(3.0) * position)
    return values * column * across * ramp_scale[:, None, None]


def draw_residual(key, part):
    return ramped_field(key, 11)


def draw_direction(key, part):
    return ramped_field(key, 23)


def draw_face_block(key, part):
    full_shape = (SUBDOMAINS, FACE_BLOCKS, BLOCK_SIZE, BLOCK_SIZE)
    mixing = jax.random.normal(jax.random.fold_in(key, 31), full_shape, jnp.float32)
    gram_part = jnp.einsum('sjab,sjcb->sjac', mixing, mixing) / BLOCK_SIZE
    low_end = 0.5
    high_end = 2.0
    diagonal = jnp.exp(jax.random.uniform(jax.random.fold_in(key, 32), full_shape[:3], jnp.float32, math.log(low_end), math.log(high_end)))
    return (gram_part + diagonal[..., None] * jnp.eye(BLOCK_SIZE, dtype=jnp.float32)).astype(jnp.bfloat16)


def draw_coarse_pattern(key, part):
    candidates = N_GRP * (2 * REACH_SUBS + 1) - 1
    row_ids = jnp.arange(SUBDOMAINS, dtype=jnp.int32)

    def one_row(row_id):
        shuffled = jax.random.permutation(jax.random.fold_in(jax.random.fold_in(key, 41), row_id), candidates)
        chosen = shuffled[:PATTERN_BLOCKS - 1].astype(jnp.int32)
        own_slot = REACH_SUBS * N_GRP + row_id % N_GRP
        chosen = chosen + (chosen >= own_slot).astype(jnp.int32)
        entry_sub = (row_id // N_GRP + chosen // N_GRP - REACH_SUBS) % N_SUB
        entries = entry_sub * N_GRP + chosen % N_GRP
        return jnp.concatenate([row_id[None], entries]).astype(jnp.int32)
    return jax.vmap(one_row)(row_ids)


def plant(values, key, least, largest):
    place = [jax.random.randint(jax.random.fold_in(key, axis), (), 0, length) for axis, length in enumerate(values.shape)]
    longest = values.shape.index(max(values.shape))
    beside = place[:longest] + [(place[longest] + 1) % values.shape[longest]] + place[longest + 1:]
    return values.at[tuple(place)].set(least).at[tuple(beside)].set(largest)


def level_of(rng, extent, pieces, least, largest):
    def one(dim, blocks):
        draws = jax.random.uniform(jax.random.fold_in(jax.random.fold_in(rng, 6), dim), (blocks,), jnp.float32, least / len(pieces), largest / len(pieces))
        return jnp.repeat(jnp.exp(draws), extent[dim] // blocks).reshape((-1,) + (1,) * (len(extent) - dim - 1))

    loudness = one(*pieces[0])
    for cut in pieces[1:]:
        loudness = loudness * one(*cut)
    return loudness


def noise(own_key, extent, width, bound, cuts=(), kind=jnp.bfloat16):
    values = jax.random.normal(own_key, extent, jnp.float32) * width
    if len(cuts) > 0:
        values = level_of(own_key, extent, cuts, -0.22, 0.18) * values
    return jnp.clip(values, min=-bound, max=bound).astype(kind)


def setup_inputs(seed: int = 0) -> dict:
    arg_keys = jax.random.split(jax.random.key(seed), 15)
    return {
        "solution": noise(arg_keys[0], (SUBDOMAINS, LOAD_CASES, 2 * FACE_SIZE), 1.0, 6.0, ((0, 128),), jnp.float32),
        "residual": draw_residual(jax.random.fold_in(arg_keys[14], 71), 0),
        "direction": draw_direction(jax.random.fold_in(arg_keys[14], 71), 0),
        "residual_product": jnp.clip(jnp.exp(jax.random.uniform(arg_keys[3], (LOAD_CASES,), jnp.float32, math.log(262144.0), math.log(5242880))), 262144.0, 5242880),
        "neighbor_slots": jax.vmap(lambda own: jax.random.permutation(own, 4))(jax.random.split(arg_keys[4], SUBDOMAINS)).reshape((SUBDOMAINS, 4)).astype(jnp.int32),
        "coupling": noise(arg_keys[5], (SUBDOMAINS, INNER_BLOCKS, 2 * BLOCK_SIZE, BLOCK_SIZE), (2 * BLOCK_SIZE) ** -0.5, 0.375, ((0, 128),)),
        "dirichlet_factor": noise(arg_keys[6], (SUBDOMAINS, INNER_BLOCKS, BLOCK_SIZE, BLOCK_SIZE), BLOCK_SIZE ** -0.5, 0.5, ((0, 128),)),
        "face_block": draw_face_block(jax.random.fold_in(arg_keys[14], 71), 0),
        "neumann_factor": noise(arg_keys[8], (SUBDOMAINS, FACE_BLOCKS, BLOCK_SIZE, BLOCK_SIZE), BLOCK_SIZE ** -0.5, 0.5, ((0, 128),)),
        "primal_block": plant(jax.random.randint(arg_keys[9], (SUBDOMAINS, PRIMALS), 0, FACE_BLOCKS), jax.random.fold_in(arg_keys[9], 1), 0, FACE_BLOCKS - 1).astype(jnp.int32),
        "primal_basis": noise(arg_keys[10], (SUBDOMAINS, PRIMALS, BLOCK_SIZE), (BLOCK_SIZE // 8) ** -0.5, 1.5, ((0, 128),)),
        "coarse_matrix": noise(arg_keys[11], (SUBDOMAINS, PATTERN_BLOCKS, PRIMALS, PRIMALS), (1.0 / (PATTERN_BLOCKS * PRIMALS) ** 0.5), 0.17677669, ((0, 128),), jnp.float32),
        "coarse_block_inverse": noise(arg_keys[12], (SUBDOMAINS, PRIMALS, PRIMALS), PRIMALS ** -0.5, 0.5, ((0, 128),), jnp.float32),
        "coarse_pattern": draw_coarse_pattern(jax.random.fold_in(arg_keys[14], 71), 0),
    }


highest_precision = lax.Precision.HIGHEST


def onehot_slots(neighbor_slots):
    return (neighbor_slots[:, :, None] == jnp.arange(4, dtype=jnp.int32)[None, None, :]).astype(jnp.float32)


def spread(owned_part, slot_onehot):
    face_width = owned_part.shape[2] // 2
    load_count = owned_part.shape[1]
    own_sub = owned_part[:, :, :face_width].reshape(N_SUB, N_GRP, load_count, face_width)
    own_grp = owned_part[:, :, face_width:].reshape(N_SUB, N_GRP, load_count, face_width)
    from_sub = jnp.roll(own_sub, 1, axis=0)
    from_grp = jnp.roll(own_grp, 1, axis=1)
    directed = jnp.stack([from_sub, own_sub, from_grp, own_grp], 2).reshape(SUBDOMAINS, 4, load_count, face_width)
    placed = jnp.einsum('sdk,sdlf->slkf', slot_onehot, directed, precision=highest_precision)
    return placed.reshape(SUBDOMAINS, load_count, FACE_BLOCKS, BLOCK_SIZE)


def collect(local_part, slot_onehot):
    load_count = local_part.shape[1]
    placed = local_part.reshape(SUBDOMAINS, load_count, 4, FACE_SIZE)
    directed = jnp.einsum('sdk,slkf->sdlf', slot_onehot, placed, precision=highest_precision)
    grid_form = directed.reshape(N_SUB, N_GRP, 4, load_count, FACE_SIZE)
    owned_sub = grid_form[:, :, 1] + jnp.roll(grid_form[:, :, 0], -1, axis=0)
    owned_grp = grid_form[:, :, 3] + jnp.roll(grid_form[:, :, 2], -1, axis=1)
    return jnp.concatenate([owned_sub, owned_grp], 3).reshape(SUBDOMAINS, load_count, 2 * FACE_SIZE)


def condensed(vector, couple, dirichlet, face_matrix):
    count_of_blocks = vector.shape[1]
    block_width = vector.shape[2]
    paired = jnp.concatenate([jnp.concatenate([vector, jnp.roll(vector, -(offset + 1), axis=1)], 2) for offset in range(3)], 1)
    interior = jnp.einsum('lib,ibk->lik', paired, couple, precision=highest_precision)
    middle = jnp.einsum('lik,ikm->lim', interior, dirichlet, precision=highest_precision)
    solved = jnp.einsum('lim,ikm->lik', middle, dirichlet, precision=highest_precision)
    returned = jnp.einsum('lik,ibk->lib', solved, couple, precision=highest_precision)
    result = jnp.einsum('ljb,jbk->ljk', vector, face_matrix, precision=highest_precision)
    for offset in range(3):
        portion = returned[:, offset * count_of_blocks:(offset + 1) * count_of_blocks]
        result = result + portion[:, :, :block_width] + jnp.roll(portion[:, :, block_width:], offset + 1, axis=1)
    return result


def apply_condensed(operands):
    vector, couple, dirichlet, face_matrix = operands
    return condensed(vector, couple.astype(jnp.float32), dirichlet.astype(jnp.float32), face_matrix.astype(jnp.float32))


def local_precondition(operands):
    halved, neumann, block_ids, basis = operands
    neumann = neumann.astype(jnp.float32)
    basis = basis.astype(jnp.float32)
    neumann_step = jnp.einsum('ljb,jbk->ljk', halved, neumann, precision=highest_precision)
    local_solve = jnp.einsum('ljk,jmk->ljm', neumann_step, neumann, precision=highest_precision)
    selector = (block_ids[:, None] == jnp.arange(halved.shape[1], dtype=jnp.int32)[None, :]).astype(jnp.float32)
    picked = jnp.einsum('ljb,cj->lcb', halved, selector, precision=highest_precision)
    coarse_residual = jnp.einsum('lcb,cb->lc', picked, basis, precision=highest_precision)
    return local_solve, coarse_residual


def spread_coarse(operands):
    coarse_correction, block_ids, basis = operands
    basis = basis.astype(jnp.float32)
    selector = (block_ids[:, None] == jnp.arange(FACE_BLOCKS, dtype=jnp.int32)[None, :]).astype(jnp.float32)
    weighted = coarse_correction[:, :, None] * basis[None]
    return jnp.einsum('lcb,cj->ljb', weighted, selector, precision=highest_precision)


def precondition(owned_part, slot_onehot, neumann_factor, primal_block, primal_basis, coarse_matrix, coarse_block_inverse, coarse_pattern):
    halved = spread(owned_part, slot_onehot) * 0.5
    local_solve, coarse_residual = lax.map(local_precondition, (halved, neumann_factor, primal_block, primal_basis))
    initial_step = jnp.einsum('pqe,pek->pqk', coarse_residual, coarse_block_inverse, precision=highest_precision)
    gathered = initial_step[coarse_pattern]
    adjacent_sum = jnp.einsum('skld,skde->sle', gathered, coarse_matrix, precision=highest_precision)
    coarse_correction = initial_step + jnp.einsum('iqc,icw->iqw', coarse_residual - adjacent_sum, coarse_block_inverse, precision=highest_precision)
    spread_back = lax.map(spread_coarse, (coarse_correction, primal_block, primal_basis))
    return collect(0.5 * (local_solve + spread_back), slot_onehot)


def reference(solution, residual, direction, residual_product, neighbor_slots, coupling, dirichlet_factor, face_block, neumann_factor, primal_block, primal_basis, coarse_matrix, coarse_block_inverse, coarse_pattern):
    slot_onehot = onehot_slots(neighbor_slots)
    local_image = lax.map(apply_condensed, (spread(direction, slot_onehot), coupling, dirichlet_factor, face_block))
    image = collect(local_image, slot_onehot)
    curvature = jnp.sum(direction * image, axis=(0, 2))
    step_length = residual_product / curvature
    new_solution = solution + step_length[None, :, None] * direction
    new_residual = residual - step_length[None, :, None] * image
    preconditioned = precondition(new_residual, slot_onehot, neumann_factor, primal_block, primal_basis, coarse_matrix, coarse_block_inverse, coarse_pattern)
    new_product = jnp.sum(new_residual * preconditioned, axis=(0, 2))
    step_ratio = new_product / residual_product
    new_direction = preconditioned + step_ratio[None, :, None] * direction
    return new_solution, new_residual, new_direction, new_product
```

```python
import functools

import jax
import jax.numpy as jnp
from jax import lax
from jax.experimental import pallas as pl
from jax.experimental.pallas import tpu as pltpu
from jax.sharding import PartitionSpec as P

F32 = jnp.float32
BF16 = jnp.bfloat16
MESH = pl.DeviceIdType.MESH

N_SUB = 32
N_GRP = 4
ROW = 8
N_X = N_SUB // ROW
W = 128
FB = 8
FACE = FB * W
REACH = 2


def split(x):
    hi = x.astype(BF16)
    lo = (x - hi.astype(F32)).astype(BF16)
    return hi, lo


def wide(x):
    return jnp.concatenate(split(x), 1)


def mm(x, w):
    return lax.dot_general(x, w, (((1,), (0,)), ((), ())), preferred_element_type=F32)


def mmt(x, w):
    return lax.dot_general(x, w, (((1,), (1,)), ((), ())), preferred_element_type=F32)


def mm3(x, w):
    xh, xl = split(x)
    wh, wl = split(w)
    return mm(jnp.concatenate([xh, xl], 1), jnp.concatenate([wh, wh], 0)) + mm(xh, wl)


def cols(b):
    return pl.ds(b * W, W)


def kernel(
    sol_hbm, res_hbm, dir_hbm, rp_ref, slots, coup_hbm, diri_hbm, face_hbm, neum_hbm, pblk_ref, basis_hbm, cmat_hbm,
    cinv_hbm, patt,
    nsol_hbm, nres_hbm, ndir_hbm, nprod_ref,
    coup, diri, face, neum, basis, cmat, cinv, sol, res,
    uf, uhl, yy, ss, c2, nr, prec, nst, nf, bms, bmr, nrel, pbm, crs, crr, cis, cir, ownc, win, cors, corr_in,
    avec, cres, z2, ar_y, ar_z, ar_x,
    lsem, osem, dsend, drecv, nsend, nrecv, bsend, brecv, crsend, crrecv, cisend, cirecv, c2send, c2recv,
    wysend, wssend, wrecv, cosend, corecv, ysend, yrecv, zsend, zrecv, xsend, xrecv,
):
    i = lax.axis_index("sub")
    g = lax.axis_index("grp")
    row = i // ROW
    col = i % ROW

    def at_sub(k):
        return lax.rem(i + k + N_SUB, N_SUB)

    def at_grp(k):
        return lax.rem(g + k + N_GRP, N_GRP)

    def dev(s, t):
        return {"sub": s, "grp": t}

    neighbor = [dev(at_sub(-1), g), dev(at_sub(1), g), dev(i, at_grp(-1)), dev(i, at_grp(1))]
    y_peers = [dev(i, at_grp(k)) for k in range(1, N_GRP)]
    z_peers = [dev(row * ROW + lax.rem(col + k, ROW), g) for k in range(1, ROW)]
    x_peers = [dev(lax.rem(row + k, N_X) * ROW + col, g) for k in range(1, N_X)]
    reach = [k for k in range(-REACH, REACH + 1) if k != 0]
    s_peers = [dev(at_sub(k), g) for k in reach]

    local = []

    def load(src, dst):
        copy = pltpu.make_async_copy(src, dst, lsem.at[len(local)])
        copy.start()
        local.append(copy)
        return copy

    l_neum = load(neum_hbm.at[0], neum)
    l_basis = load(basis_hbm.at[0], basis)
    l_dir = [load(dir_hbm.at[0, :, pl.ds(f * FACE, FACE)], uf.at[2 * f + 1]) for f in range(2)]
    l_res = [load(res_hbm.at[0, :, pl.ds(f * FACE, FACE)], res.at[f]) for f in range(2)]
    l_face = load(face_hbm.at[0], face)
    l_coup = load(coup_hbm.at[0], coup)
    l_diri = load(diri_hbm.at[0], diri)
    l_cinv = load(cinv_hbm.at[0], cinv)
    l_cmat = load(cmat_hbm.at[0], cmat)
    l_sol = [load(sol_hbm.at[0, :, pl.ds(f * FACE, FACE)], sol.at[f]) for f in range(2)]

    barrier = pltpu.get_barrier_semaphore()
    everyone = y_peers + z_peers + x_peers + s_peers
    for peer in everyone:
        pl.semaphore_signal(barrier, inc=1, device_id=peer, device_id_type=MESH)
    pl.semaphore_wait(barrier, len(everyone))

    sent = []

    def send(src, dst, send_sem, recv_sem, peer):
        copy = pltpu.make_async_remote_copy(
            src_ref=src, dst_ref=dst, send_sem=send_sem, recv_sem=recv_sem, device_id=peer, device_id_type=MESH
        )
        copy.start()
        sent.append(copy)

    def arrived(ref, send_sem, recv_sem):
        pltpu.make_async_remote_copy(
            src_ref=ref, dst_ref=ref, send_sem=send_sem, recv_sem=recv_sem, device_id=neighbor[0], device_id_type=MESH
        ).wait_recv()

    for f in (1, 0):
        send(
            dir_hbm.at[0, :, pl.ds(f * FACE, FACE)], uf.at[2 * f], dsend.at[f], drecv.at[f], neighbor[2 * f + 1]
        )

    l_basis.wait()
    pb_row = pblk_ref[...].astype(F32)
    pbm[...] = jnp.transpose(jnp.broadcast_to(pb_row, (W, W)))
    basis_f = basis[...].astype(F32)
    for d in range(4):
        base = (slots[0, d] * FB).astype(F32)
        bms[d, 0:W, :] = basis_f
        bms[d, W : W + 8, :] = jnp.broadcast_to(pb_row - base, (8, W))
        send(bms.at[d], bmr.at[d ^ 1], bsend.at[d], brecv.at[d ^ 1], neighbor[d])

    l_neum.wait()
    for f in (1, 0):
        start = slots[0, 2 * f] * FB

        def to_f32(b, carry, f=f, start=start):
            nst[f, b] = neum[start + b].astype(F32)
            return carry

        lax.fori_loop(0, FB, to_f32, 0)
        send(nst.at[f], nf.at[f], nsend.at[f], nrecv.at[f], neighbor[2 * f])

    for d in range(4):
        arrived(bmr.at[d], bsend.at[d], brecv.at[d])
        nrel[d] = jnp.transpose(jnp.broadcast_to(bmr[d, W : W + 1, :], (W, W)))

    def own_mask(d, b):
        number = (slots[0, d] * FB + b).astype(F32)
        return jnp.where(pbm[...] == number, basis[...].astype(F32), 0.0).astype(BF16)

    def nb_mask(d, b):
        return jnp.where(nrel[d] == float(b), bmr[d, 0:W, :], 0.0).astype(BF16)

    def coarse_pair(read, d):
        total = None
        for b in range(FB):
            both = jnp.concatenate([own_mask(d, b), nb_mask(d, b)], 0)
            part = mmt(wide(read(b)), jnp.concatenate([both, both], 1))
            total = part if total is None else total + part
        return total

    for copy in l_res:
        copy.wait()
    ownc[...] = jnp.zeros_like(ownc)

    def coarse_of_residual(f, carry):
        pair = coarse_pair(lambda b: res[f, :, cols(b)], 2 * f + 1)
        ownc[0] += pair[:, :W]
        crs[f] = pair[:, W:]
        return carry

    lax.fori_loop(0, 2, coarse_of_residual, 0)
    for f in range(2):
        send(crs.at[f], crr.at[f], crsend.at[f], crrecv.at[f], neighbor[2 * f + 1])

    for copy in l_dir:
        copy.wait()
    l_face.wait()
    l_coup.wait()
    l_diri.wait()

    def interior(jobs):
        first = []
        for lhs, n in jobs:
            two = mm(lhs, coup[n])
            first.append(wide(two[:W] + two[W:]))
        second = []
        for x, (_, n) in zip(first, jobs):
            m = diri[n]
            second.append(wide(mm(x, jnp.concatenate([m, m], 0))))
        third = []
        for x, (_, n) in zip(second, jobs):
            m = diri[n]
            third.append(wide(mmt(x, jnp.concatenate([m, m], 1))))
        out = []
        for x, (_, n) in zip(third, jobs):
            m = coup[n]
            out.append(mmt(x, jnp.concatenate([m, m], 1)))
        return out

    inside = [(q, b) for q in range(3) for b in range(FB - 1 - q)]

    def one_direction(step, carry):
        d = lax.rem(2 * step + 1, 5)

        @pl.when(step == 2)
        def _():
            arrived(uf.at[0], dsend.at[0], drecv.at[0])

        @pl.when(step == 3)
        def _():
            arrived(uf.at[2], dsend.at[1], drecv.at[1])

        base = slots[0, d] * FB
        for b in range(FB):
            hi, lo = split(uf[d, :, cols(b)])
            uhl[d, 0:W, cols(b)] = hi
            uhl[d, W : 2 * W, cols(b)] = lo
            m = face[base + b]
            yy[d, :, cols(b)] = mm(jnp.concatenate([hi, lo], 1), jnp.concatenate([m, m], 0))
        for k in range(0, len(inside), 6):
            group = inside[k : k + 6]
            jobs = [
                (
                    jnp.concatenate([uhl[d, :, cols(b)], uhl[d, :, cols(b + q + 1)]], 1),
                    q * 4 * FB + base + b,
                )
                for q, b in group
            ]
            for (q, b), out in zip(group, interior(jobs)):
                yy[d, :, cols(b)] += out[:, :W]
                yy[d, :, cols(b + q + 1)] += out[:, W:]
        return carry

    lax.fori_loop(0, 4, one_direction, 0)

    def direction_of(slot):
        where = jnp.int32(0)
        for d in range(1, 4):
            where = jnp.where(slots[0, d] == slot, jnp.int32(d), where)
        return where

    across = [(q, b) for q in range(3) for b in range(FB - 1 - q, FB)]

    def straddling(d, carry):
        slot = slots[0, d]
        after = direction_of(lax.rem(slot + 1, 4))
        jobs = [
            (
                jnp.concatenate([uhl[d, :, cols(b)], uhl[after, :, cols(b + q + 1 - FB)]], 1),
                q * 4 * FB + slot * FB + b,
            )
            for q, b in across
        ]
        tails = [None] * 3
        for (q, b), out in zip(across, interior(jobs)):
            yy[d, :, cols(b)] += out[:, :W]
            m = b + q + 1 - FB
            tails[m] = out[:, W:] if tails[m] is None else tails[m] + out[:, W:]
        for m in range(3):
            ss[d, :, cols(m)] = tails[m]
        return carry

    lax.fori_loop(0, 4, straddling, 0)

    for d in range(4):
        before = direction_of(lax.rem(slots[0, d] + 3, 4))
        for m in range(3):
            yy[d, :, cols(m)] += ss[before, :, cols(m)]

    for f in (1, 0):
        send(yy.at[2 * f], c2.at[f], c2send.at[f], c2recv.at[f], neighbor[2 * f])

    def folded(x):
        return jnp.sum(jnp.transpose(x).reshape(W // 8, 8, W), axis=0)

    stages = (
        (ar_y, ysend, yrecv, N_GRP, g, y_peers),
        (ar_z, zsend, zrecv, ROW, col, z_peers),
        (ar_x, xsend, xrecv, N_X, row, x_peers),
    )

    def stage_send(which, stage, value):
        buf, ssem, rsem, count, me, peers = stages[stage]
        buf[which, me] = value
        for k, peer in enumerate(peers):
            send(buf.at[which, me], buf.at[which, me], ssem.at[which, k], rsem.at[which, me], peer)

    def stage_wait(which, stage):
        buf, ssem, rsem, count, me, peers = stages[stage]
        for k in range(1, count):
            other = lax.rem(me + k, count)
            arrived(buf.at[which, other], ssem.at[which, 0], rsem.at[which, other])
        total = buf[which, 0]
        for k in range(1, count):
            total = total + buf[which, k]
        return total

    def curve(d, acc):
        for b in range(FB):
            acc = acc + uf[d, :, cols(b)] * yy[d, :, cols(b)]
        return acc

    stage_send(0, 0, folded(lax.fori_loop(0, 4, curve, jnp.zeros((W, W), F32))))

    def coarse_of_image(d, carry):
        pair = coarse_pair(lambda b: yy[d, :, cols(b)], d)
        ownc[1] += pair[:, :W]
        cis[d] = pair[:, W:]
        return carry

    lax.fori_loop(0, 4, coarse_of_image, 0)
    for d in (2, 3, 0, 1):
        send(cis.at[d], cir.at[d ^ 1], cisend.at[d], cirecv.at[d ^ 1], neighbor[d])

    stage_send(0, 1, stage_wait(0, 0))
    stage_send(0, 2, stage_wait(0, 1))
    rp_row = rp_ref[...]
    curvature = jnp.sum(stage_wait(0, 2), axis=0, keepdims=True)
    avec[...] = jnp.transpose(jnp.broadcast_to(rp_row / curvature, (W, W)))

    for f in range(2):
        arrived(crr.at[f], crsend.at[f], crrecv.at[f])
    for d in range(4):
        arrived(cir.at[d], cisend.at[d], cirecv.at[d])
    l_cinv.wait()
    image_part = ownc[1] + ((cir[0] + cir[1]) + (cir[2] + cir[3]))
    residual_part = ownc[0] + (crr[0] + crr[1])
    cres[0] = 0.5 * (residual_part - avec[...] * image_part)
    win[REACH, g] = mm3(cres[0], cinv[...])
    for k, peer in enumerate(y_peers):
        send(win.at[REACH, g], win.at[REACH, g], wysend.at[k], wrecv.at[REACH, g], peer)

    def forward(k):
        piece = at_grp(k)
        for n, (step, peer) in enumerate(zip(reach, s_peers)):
            send(
                win.at[REACH, piece], win.at[REACH - step, piece], wssend.at[k, n], wrecv.at[REACH - step, piece], peer
            )

    forward(0)

    for copy in l_sol:
        copy.wait()
    outs = []

    def store(src, dst):
        copy = pltpu.make_async_copy(src, dst, osem.at[len(outs)])
        copy.start()
        outs.append(copy)

    z2[...] = jnp.zeros_like(z2)

    def own_face(f):
        a = avec[...]
        base = slots[0, 2 * f + 1] * FB
        acc = z2[...]
        for b in range(FB):
            sol[f, :, cols(b)] += a * uf[2 * f + 1, :, cols(b)]
            new = res[f, :, cols(b)] - a * (yy[2 * f + 1, :, cols(b)] + c2[f, :, cols(b)])
            nr[f, :, cols(b)] = new
            mine = neum[base + b]
            theirs = nf[f, b].astype(BF16)
            both = jnp.concatenate([mine, theirs], 1)
            z = mm(wide(0.5 * new), jnp.concatenate([both, both], 0))
            acc = acc + (z[:, :W] * z[:, :W] + z[:, W:] * z[:, W:])
            lhs = jnp.concatenate([wide(z[:, :W]), wide(z[:, W:])], 1)
            prec[f, :, cols(b)] = mmt(lhs, jnp.concatenate([mine, mine, theirs, theirs], 1))
        z2[...] = acc

    arrived(c2.at[0], c2send.at[0], c2recv.at[0])
    arrived(nf.at[0], nsend.at[0], nrecv.at[0])
    own_face(0)
    for k in range(1, N_GRP):
        piece = at_grp(k)
        arrived(win.at[REACH, piece], wysend.at[0], wrecv.at[REACH, piece])
        forward(k)
    arrived(c2.at[1], c2send.at[1], c2recv.at[1])
    arrived(nf.at[1], nsend.at[1], nrecv.at[1])
    own_face(1)
    for f in range(2):
        store(sol.at[f], nsol_hbm.at[0, :, pl.ds(f * FACE, FACE)])
        store(nr.at[f], nres_hbm.at[0, :, pl.ds(f * FACE, FACE)])

    for k in range(N_GRP):
        piece = at_grp(k)
        for step in reach:
            arrived(win.at[REACH - step, piece], wssend.at[0, 0], wrecv.at[REACH - step, piece])
    l_cmat.wait()
    adjacent = None
    for k in range(9):
        entry = patt[0, k]
        place = jnp.minimum(lax.rem(entry // N_GRP - i + REACH + N_SUB, N_SUB), 2 * REACH)
        part = mm3(win[place, lax.rem(entry, N_GRP)], cmat[k])
        adjacent = part if adjacent is None else adjacent + part
    corr = win[REACH, g] + mm3(cres[0] - adjacent, cinv[...])
    cors[...] = corr
    for f in (1, 0):
        send(cors, corr_in.at[f], cosend.at[f], corecv.at[f], neighbor[2 * f])
    stage_send(1, 0, folded(z2[...] + corr * cres[0]))

    mine_w = wide(corr)
    for f in range(2):
        arrived(corr_in.at[f], cosend.at[f], corecv.at[f])

    def spread_back(f, carry):
        lhs = jnp.concatenate([wide(cors[...]), wide(corr_in[f])], 1)
        for b in range(FB):
            own = own_mask(2 * f + 1, b)
            other = nb_mask(2 * f + 1, b)
            back = mm(lhs, jnp.concatenate([own, own, other, other], 0))
            prec[f, :, cols(b)] = 0.5 * (prec[f, :, cols(b)] + back)
        return carry

    lax.fori_loop(0, 2, spread_back, 0)

    stage_send(1, 1, stage_wait(1, 0))
    stage_send(1, 2, stage_wait(1, 1))
    product = jnp.sum(stage_wait(1, 2), axis=0, keepdims=True)
    nprod_ref[...] = product
    avec[...] = jnp.transpose(jnp.broadcast_to(product / rp_row, (W, W)))

    def new_direction(f, carry):
        a = avec[...]
        for b in range(FB):
            prec[f, :, cols(b)] += a * uf[2 * f + 1, :, cols(b)]
        return carry

    lax.fori_loop(0, 2, new_direction, 0)
    for f in range(2):
        store(prec.at[f], ndir_hbm.at[0, :, pl.ds(f * FACE, FACE)])
    for copy in sent:
        copy.wait_send()
    for copy in outs:
        copy.wait()


def shards(
    solution,
    residual,
    direction,
    residual_product,
    neighbor_slots,
    coupling,
    dirichlet_factor,
    face_block,
    neumann_factor,
    primal_block,
    primal_basis,
    coarse_matrix,
    coarse_block_inverse,
    coarse_pattern,
):
    hbm = pl.BlockSpec(memory_space=pl.ANY)
    vmem = pl.BlockSpec(memory_space=pltpu.VMEM)
    smem = pl.BlockSpec(memory_space=pltpu.SMEM)
    dma = pltpu.SemaphoreType.DMA
    big = jax.ShapeDtypeStruct((1, W, 2 * FACE), F32)
    nsol, nres, ndir, nprod = pl.pallas_call(
        kernel,
        out_shape=(big, big, big, jax.ShapeDtypeStruct((1, W), F32)),
        in_specs=[hbm, hbm, hbm, vmem, smem, hbm, hbm, hbm, hbm, vmem, hbm, hbm, hbm, smem],
        out_specs=(hbm, hbm, hbm, vmem),
        scratch_shapes=[
            pltpu.VMEM((96, 2 * W, W), BF16),
            pltpu.VMEM((96, W, W), BF16),
            pltpu.VMEM((32, W, W), BF16),
            pltpu.VMEM((32, W, W), BF16),
            pltpu.VMEM((W, W), BF16),
            pltpu.VMEM((9, W, W), F32),
            pltpu.VMEM((W, W), F32),
            pltpu.VMEM((2, W, FACE), F32),
            pltpu.VMEM((2, W, FACE), F32),
            pltpu.VMEM((4, W, FACE), F32),
            pltpu.VMEM((4, 2 * W, FACE), BF16),
            pltpu.VMEM((4, W, FACE), F32),
            pltpu.VMEM((4, W, 3 * W), F32),
            pltpu.VMEM((2, W, FACE), F32),
            pltpu.VMEM((2, W, FACE), F32),
            pltpu.VMEM((2, W, FACE), F32),
            pltpu.VMEM((2, FB, W, W), F32),
            pltpu.VMEM((2, FB, W, W), F32),
            pltpu.VMEM((4, W + 8, W), F32),
            pltpu.VMEM((4, W + 8, W), F32),
            pltpu.VMEM((4, W, W), F32),
            pltpu.VMEM((W, W), F32),
            pltpu.VMEM((2, W, W), F32),
            pltpu.VMEM((2, W, W), F32),
            pltpu.VMEM((4, W, W), F32),
            pltpu.VMEM((4, W, W), F32),
            pltpu.VMEM((2, W, W), F32),
            pltpu.VMEM((2 * REACH + 1, N_GRP, W, W), F32),
            pltpu.VMEM((W, W), F32),
            pltpu.VMEM((2, W, W), F32),
            pltpu.VMEM((W, W), F32),
            pltpu.VMEM((1, W, W), F32),
            pltpu.VMEM((W, W), F32),
            pltpu.VMEM((2, N_GRP, 8, W), F32),
            pltpu.VMEM((2, ROW, 8, W), F32),
            pltpu.VMEM((2, N_X, 8, W), F32),
            dma((13,)),
            dma((6,)),
            dma((2,)), dma((2,)),
            dma((2,)), dma((2,)),
            dma((4,)), dma((4,)),
            dma((2,)), dma((2,)),
            dma((4,)), dma((4,)),
            dma((2,)), dma((2,)),
            dma((3,)), dma((N_GRP, 4)), dma((2 * REACH + 1, N_GRP)),
            dma((2,)), dma((2,)),
            dma((2, 3)), dma((2, N_GRP)),
            dma((2, 7)), dma((2, ROW)),
            dma((2, 3)), dma((2, N_X)),
        ],
        compiler_params=pltpu.CompilerParams(
            collective_id=0, has_side_effects=True, vmem_limit_bytes=60 * 1024 * 1024
        ),
        name="pcg_step",
    )(
        solution,
        residual,
        direction,
        residual_product.reshape(1, W),
        neighbor_slots,
        coupling,
        dirichlet_factor,
        face_block,
        neumann_factor,
        primal_block,
        primal_basis,
        coarse_matrix,
        coarse_block_inverse,
        coarse_pattern,
    )
    return nsol, nres, ndir, nprod.reshape(W)


def solution(mesh):
    both = ("sub", "grp")

    def split_first(rank):
        return P(both, *([None] * (rank - 1)))

    return jax.shard_map(
        shards,
        mesh=mesh,
        in_specs=(
            split_first(3), split_first(3), split_first(3), P(), split_first(2), split_first(4), split_first(4),
            split_first(4), split_first(4), split_first(2), split_first(3), split_first(4), split_first(3),
            split_first(2),
        ),
        out_specs=(split_first(3), split_first(3), split_first(3), P()),
        check_vma=False,
    )
```

```python
import functools

import jax
import jax.numpy as jnp
from jax import lax
from jax.experimental import pallas as pl
from jax.experimental.pallas import tpu as pltpu
from jax.sharding import PartitionSpec as P

F32 = jnp.float32
BF16 = jnp.bfloat16
MESH = pl.DeviceIdType.MESH

N_SUB = 32
N_GRP = 4
ROW = 8
N_X = N_SUB // ROW
W = 128
FB = 8
FACE = FB * W
REACH = 2


def split(x):
    hi = x.astype(BF16)
    lo = (x - hi.astype(F32)).astype(BF16)
    return hi, lo


def wide(x):
    return jnp.concatenate(split(x), 1)


def mm(x, w):
    return lax.dot_general(x, w, (((1,), (0,)), ((), ())), preferred_element_type=F32)


def mmt(x, w):
    return lax.dot_general(x, w, (((1,), (1,)), ((), ())), preferred_element_type=F32)


def mm3(x, w):
    xh, xl = split(x)
    wh, wl = split(w)
    return mm(jnp.concatenate([xh, xl], 1), jnp.concatenate([wh, wh], 0)) + mm(xh, wl)


def cols(b):
    return pl.ds(b * W, W)


def kernel(
    res_hbm, dir_hbm, rp_ref, slots, coup_hbm, diri_hbm, face_hbm, neum_hbm, pblk_ref, basis_hbm, cmat_hbm,
    cinv_hbm, patt,
    nr_hbm, prec_hbm, rows_ref,
    coup, diri, face, neum, basis, cmat, cinv, res,
    uf, uhl, yy, tt, ss, c2, nr, prec, nst, nf, bms, bmr, nrel, pbm, crs, crr, cis, cir, ownc, win, cors, corr_in,
    avec, cres, z2, ar_y, ar_z, ar_x,
    lsem, osem, dsend, drecv, nsend, nrecv, bsend, brecv, crsend, crrecv, cisend, cirecv, c2send, c2recv,
    wysend, wssend, wrecv, cosend, corecv, ysend, yrecv, zsend, zrecv, xsend, xrecv,
):
    i = lax.axis_index("sub")
    g = lax.axis_index("grp")
    row = i // ROW
    col = i % ROW

    def at_sub(k):
        return lax.rem(i + k + N_SUB, N_SUB)

    def at_grp(k):
        return lax.rem(g + k + N_GRP, N_GRP)

    def dev(s, t):
        return {"sub": s, "grp": t}

    neighbor = [dev(at_sub(-1), g), dev(at_sub(1), g), dev(i, at_grp(-1)), dev(i, at_grp(1))]
    y_peers = [dev(i, at_grp(k)) for k in range(1, N_GRP)]
    z_peers = [dev(row * ROW + lax.rem(col + k, ROW), g) for k in range(1, ROW)]
    x_peers = [dev(lax.rem(row + k, N_X) * ROW + col, g) for k in range(1, N_X)]
    reach = [k for k in range(-REACH, REACH + 1) if k != 0]
    s_peers = [dev(at_sub(k), g) for k in reach]

    local = []

    def load(src, dst):
        copy = pltpu.make_async_copy(src, dst, lsem.at[len(local)])
        copy.start()
        local.append(copy)
        return copy

    l_neum = load(neum_hbm.at[0], neum)
    l_basis = load(basis_hbm.at[0], basis)
    l_dir = [load(dir_hbm.at[0, :, pl.ds(f * FACE, FACE)], uf.at[2 * f + 1]) for f in range(2)]
    l_res = [load(res_hbm.at[0, :, pl.ds(f * FACE, FACE)], res.at[f]) for f in range(2)]
    l_face = load(face_hbm.at[0], face)
    l_coup = load(coup_hbm.at[0], coup)
    l_diri = load(diri_hbm.at[0], diri)
    l_cinv = load(cinv_hbm.at[0], cinv)
    l_cmat = load(cmat_hbm.at[0], cmat)

    barrier = pltpu.get_barrier_semaphore()
    everyone = y_peers + z_peers + x_peers + s_peers
    for peer in everyone:
        pl.semaphore_signal(barrier, inc=1, device_id=peer, device_id_type=MESH)
    pl.semaphore_wait(barrier, len(everyone))

    sent = []

    def send(src, dst, send_sem, recv_sem, peer):
        copy = pltpu.make_async_remote_copy(
            src_ref=src, dst_ref=dst, send_sem=send_sem, recv_sem=recv_sem, device_id=peer, device_id_type=MESH
        )
        copy.start()
        sent.append(copy)

    def arrived(ref, send_sem, recv_sem):
        pltpu.make_async_remote_copy(
            src_ref=ref, dst_ref=ref, send_sem=send_sem, recv_sem=recv_sem, device_id=neighbor[0], device_id_type=MESH
        ).wait_recv()

    half = FACE // 2
    for h in range(2):
        send(
            dir_hbm.at[0, :, pl.ds(FACE + h * half, half)], uf.at[2, :, pl.ds(h * half, half)],
            dsend.at[h], drecv.at[h], neighbor[3],
        )
    send(dir_hbm.at[0, :, pl.ds(0, FACE)], uf.at[0], dsend.at[2], drecv.at[2], neighbor[1])

    l_basis.wait()
    pb_row = pblk_ref[...].astype(F32)
    pbm[...] = jnp.transpose(jnp.broadcast_to(pb_row, (W, W)))
    basis_f = basis[...].astype(F32)
    for d in range(4):
        bms[d, 0:W, :] = basis_f
        bms[d, W : W + 8, :] = jnp.broadcast_to(pb_row - (slots[0, d] * FB).astype(F32), (8, W))

    def send_basis(d):
        send(bms.at[d], bmr.at[d ^ 1], bsend.at[d], brecv.at[d ^ 1], neighbor[d])

    def basis_arrived(d):
        arrived(bmr.at[d], bsend.at[d], brecv.at[d])
        nrel[d] = jnp.transpose(jnp.broadcast_to(bmr[d, W : W + 1, :], (W, W)))

    send_basis(2)
    send_basis(0)
    l_neum.wait()
    for f in (1, 0):
        start = slots[0, 2 * f] * FB

        def to_f32(b, carry, f=f, start=start):
            nst[f, b] = neum[start + b].astype(F32)
            return carry

        lax.fori_loop(0, FB, to_f32, 0)
        send(nst.at[f], nf.at[f], nsend.at[f], nrecv.at[f], neighbor[2 * f])
    send_basis(3)
    send_basis(1)

    def own_mask(d, b):
        number = (slots[0, d] * FB + b).astype(F32)
        return jnp.where(pbm[...] == number, basis[...].astype(F32), 0.0).astype(BF16)

    def nb_mask(d, b):
        return jnp.where(nrel[d] == float(b), bmr[d, 0:W, :], 0.0).astype(BF16)

    def coarse_pair(read, d):
        total = None
        for b in range(FB):
            both = jnp.concatenate([own_mask(d, b), nb_mask(d, b)], 0)
            part = mmt(wide(read(b)), jnp.concatenate([both, both], 1))
            total = part if total is None else total + part
        return total

    for copy in l_dir:
        copy.wait()
    l_face.wait()
    l_coup.wait()
    l_diri.wait()

    def interior(jobs):
        first = []
        for lhs, n in jobs:
            two = mm(lhs, coup[n])
            first.append(wide(two[:W] + two[W:]))
        second = []
        for x, (_, n) in zip(first, jobs):
            m = diri[n]
            second.append(wide(mm(x, jnp.concatenate([m, m], 0))))
        third = []
        for x, (_, n) in zip(second, jobs):
            m = diri[n]
            third.append(wide(mmt(x, jnp.concatenate([m, m], 1))))
        out = []
        for x, (_, n) in zip(third, jobs):
            m = coup[n]
            out.append(mmt(x, jnp.concatenate([m, m], 1)))
        return out

    def face_term(d, blocks):
        base = slots[0, d] * FB
        for b in blocks:
            hi, lo = split(uf[d, :, cols(b)])
            uhl[d, 0:W, cols(b)] = hi
            uhl[d, W : 2 * W, cols(b)] = lo
            m = face[base + b]
            yy[d, :, cols(b)] = mm(jnp.concatenate([hi, lo], 1), jnp.concatenate([m, m], 0))

    def within(d, pairs):
        base = slots[0, d] * FB
        for k in range(0, len(pairs), 6):
            group = pairs[k : k + 6]
            jobs = [
                (
                    jnp.concatenate([uhl[d, :, cols(b)], uhl[d, :, cols(b + q + 1)]], 1),
                    q * 4 * FB + base + b,
                )
                for q, b in group
            ]
            for (q, b), out in zip(group, interior(jobs)):
                yy[d, :, cols(b)] += out[:, :W]
                yy[d, :, cols(b + q + 1)] += out[:, W:]

    inside = [(q, b) for q in range(3) for b in range(FB - 1 - q)]
    early = [(q, b) for q, b in inside if b + q + 1 < FB // 2]
    late = [(q, b) for q, b in inside if b + q + 1 >= FB // 2]
    across = [(q, b) for q in range(3) for b in range(FB - 1 - q, FB)]

    def direction_of(slot):
        where = jnp.int32(0)
        for d in range(1, 4):
            where = jnp.where(slots[0, d] == slot, jnp.int32(d), where)
        return where

    def straddling(p, carry):
        slot = lax.rem(slots[0, 2] + 1 + p, 4)
        this = direction_of(slot)
        after = direction_of(lax.rem(slot + 1, 4))
        jobs = [
            (
                jnp.concatenate([uhl[this, :, cols(b)], uhl[after, :, cols(b + q + 1 - FB)]], 1),
                q * 4 * FB + slot * FB + b,
            )
            for q, b in across
        ]
        heads, tails = [None] * 3, [None] * 3
        for (q, b), out in zip(across, interior(jobs)):
            h, m = b - FB + 3, b + q + 1 - FB
            heads[h] = out[:, :W] if heads[h] is None else heads[h] + out[:, :W]
            tails[m] = out[:, W:] if tails[m] is None else tails[m] + out[:, W:]
        for m in range(3):
            tt[p, :, cols(m)] = heads[m]
            ss[p, :, cols(m)] = tails[m]
        return carry

    def first_three(step, carry):
        d = lax.rem(2 * step + 1, 5)

        @pl.when(step == 2)
        def _():
            arrived(uf.at[0], dsend.at[2], drecv.at[2])

        face_term(d, range(FB))
        within(d, inside)
        return carry

    lax.fori_loop(0, 3, first_three, 0)
    lax.fori_loop(0, 2, straddling, 0)

    basis_arrived(3)
    basis_arrived(1)
    for copy in l_res:
        copy.wait()
    ownc[...] = jnp.zeros_like(ownc)

    def coarse_of_residual(f, carry):
        pair = coarse_pair(lambda b: res[f, :, cols(b)], 2 * f + 1)
        ownc[0] += pair[:, :W]
        crs[f] = pair[:, W:]
        return carry

    lax.fori_loop(0, 2, coarse_of_residual, 0)
    for f in range(2):
        send(crs.at[f], crr.at[f], crsend.at[f], crrecv.at[f], neighbor[2 * f + 1])

    arrived(uf.at[2, :, pl.ds(0, half)], dsend.at[0], drecv.at[0])
    face_term(2, range(FB // 2))
    within(2, early)
    straddling(2, 0)
    arrived(uf.at[2, :, pl.ds(half, half)], dsend.at[1], drecv.at[1])
    face_term(2, range(FB // 2, FB))
    within(2, late)
    straddling(3, 0)
    for d in range(4):
        place = lax.rem(slots[0, d] - slots[0, 2] + 7, 4)
        before = lax.rem(slots[0, d] - slots[0, 2] + 6, 4)
        for m in range(3):
            yy[d, :, cols(m)] += ss[before, :, cols(m)]
            yy[d, :, cols(FB - 3 + m)] += tt[place, :, cols(m)]

    def folded(x):
        return jnp.sum(jnp.transpose(x).reshape(W // 8, 8, W), axis=0)

    stages = (
        (ar_y, ysend, yrecv, N_GRP, g, y_peers),
        (ar_z, zsend, zrecv, ROW, col, z_peers),
        (ar_x, xsend, xrecv, N_X, row, x_peers),
    )

    def stage_send(which, stage, value):
        buf, ssem, rsem, count, me, peers = stages[stage]
        buf[which, me] = value
        for k, peer in enumerate(peers):
            send(buf.at[which, me], buf.at[which, me], ssem.at[which, k], rsem.at[which, me], peer)

    def stage_wait(which, stage):
        buf, ssem, rsem, count, me, peers = stages[stage]
        for k in range(1, count):
            other = lax.rem(me + k, count)
            arrived(buf.at[which, other], ssem.at[which, 0], rsem.at[which, other])
        total = buf[which, 0]
        for k in range(1, count):
            total = total + buf[which, k]
        return total

    def curve(d, acc):
        for b in range(FB):
            acc = acc + uf[d, :, cols(b)] * yy[d, :, cols(b)]
        return acc

    stage_send(0, 0, folded(lax.fori_loop(0, 4, curve, jnp.zeros((W, W), F32))))

    basis_arrived(0)
    basis_arrived(2)

    def coarse_of_image(k, carry):
        d = lax.rem(k + 2, 4)
        pair = coarse_pair(lambda b: yy[d, :, cols(b)], d)
        ownc[1] += pair[:, :W]
        cis[d] = pair[:, W:]
        return carry

    lax.fori_loop(0, 2, coarse_of_image, 0)
    for d in (2, 3):
        send(cis.at[d], cir.at[d ^ 1], cisend.at[d], cirecv.at[d ^ 1], neighbor[d])
    lax.fori_loop(2, 4, coarse_of_image, 0)
    for d in (0, 1):
        send(cis.at[d], cir.at[d ^ 1], cisend.at[d], cirecv.at[d ^ 1], neighbor[d])

    quarter = FACE // 4

    def return_piece(f, k):
        piece = pl.ds(k * quarter, quarter)
        send(
            yy.at[2 * f, :, piece], c2.at[f, :, piece], c2send.at[f, k], c2recv.at[f, k], neighbor[2 * f]
        )

    def returned(f):
        for k in range(4):
            piece = pl.ds(k * quarter, quarter)
            arrived(c2.at[f, :, piece], c2send.at[f, k], c2recv.at[f, k])

    stage_send(0, 1, stage_wait(0, 0))
    return_piece(1, 0)
    return_piece(1, 1)
    stage_send(0, 2, stage_wait(0, 1))
    for k in range(4):
        return_piece(0, k)
    rp_row = rp_ref[...]
    curvature = jnp.sum(stage_wait(0, 2), axis=0, keepdims=True)
    step_row = rp_row / curvature
    avec[...] = jnp.transpose(jnp.broadcast_to(step_row, (W, W)))

    for f in range(2):
        arrived(crr.at[f], crsend.at[f], crrecv.at[f])
    for d in range(4):
        arrived(cir.at[d], cisend.at[d], cirecv.at[d])
    l_cinv.wait()
    image_part = ownc[1] + ((cir[0] + cir[1]) + (cir[2] + cir[3]))
    residual_part = ownc[0] + (crr[0] + crr[1])
    cres[0] = 0.5 * (residual_part - avec[...] * image_part)
    win[REACH, g] = mm3(cres[0], cinv[...])
    for k, peer in enumerate(y_peers):
        send(win.at[REACH, g], win.at[REACH, g], wysend.at[k], wrecv.at[REACH, g], peer)

    def forward(k):
        piece = at_grp(k)
        for n, (step, peer) in enumerate(zip(reach, s_peers)):
            send(
                win.at[REACH, piece], win.at[REACH - step, piece], wssend.at[k, n], wrecv.at[REACH - step, piece], peer
            )

    forward(0)
    return_piece(1, 2)
    return_piece(1, 3)

    outs = []

    def store(src, dst):
        copy = pltpu.make_async_copy(src, dst, osem.at[len(outs)])
        copy.start()
        outs.append(copy)

    z2[...] = jnp.zeros_like(z2)

    def own_face(f):
        a = avec[...]
        base = slots[0, 2 * f + 1] * FB
        acc = z2[...]
        for b in range(FB):
            new = res[f, :, cols(b)] - a * (yy[2 * f + 1, :, cols(b)] + c2[f, :, cols(b)])
            nr[f, :, cols(b)] = new
            mine = neum[base + b]
            theirs = nf[f, b].astype(BF16)
            both = jnp.concatenate([mine, theirs], 1)
            z = mm(wide(0.5 * new), jnp.concatenate([both, both], 0))
            acc = acc + (z[:, :W] * z[:, :W] + z[:, W:] * z[:, W:])
            lhs = jnp.concatenate([wide(z[:, :W]), wide(z[:, W:])], 1)
            prec[f, :, cols(b)] = mmt(lhs, jnp.concatenate([mine, mine, theirs, theirs], 1))
        z2[...] = acc

    returned(0)
    arrived(nf.at[0], nsend.at[0], nrecv.at[0])
    own_face(0)
    for k in range(1, N_GRP):
        piece = at_grp(k)
        arrived(win.at[REACH, piece], wysend.at[0], wrecv.at[REACH, piece])
        forward(k)
    returned(1)
    arrived(nf.at[1], nsend.at[1], nrecv.at[1])
    own_face(1)
    for f in range(2):
        store(nr.at[f], nr_hbm.at[f])

    for k in range(N_GRP):
        piece = at_grp(k)
        for step in reach:
            arrived(win.at[REACH - step, piece], wssend.at[0, 0], wrecv.at[REACH - step, piece])
    l_cmat.wait()
    adjacent = None
    for k in range(9):
        entry = patt[0, k]
        place = jnp.minimum(lax.rem(entry // N_GRP - i + REACH + N_SUB, N_SUB), 2 * REACH)
        part = mm3(win[place, lax.rem(entry, N_GRP)], cmat[k])
        adjacent = part if adjacent is None else adjacent + part
    corr = win[REACH, g] + mm3(cres[0] - adjacent, cinv[...])
    cors[...] = corr
    for f in (1, 0):
        send(cors, corr_in.at[f], cosend.at[f], corecv.at[f], neighbor[2 * f])
    stage_send(1, 0, folded(z2[...] + corr * cres[0]))

    mine_w = wide(corr)
    for f in range(2):
        arrived(corr_in.at[f], cosend.at[f], corecv.at[f])

    def spread_back(f, carry):
        lhs = jnp.concatenate([wide(cors[...]), wide(corr_in[f])], 1)
        for b in range(FB):
            own = own_mask(2 * f + 1, b)
            other = nb_mask(2 * f + 1, b)
            back = mm(lhs, jnp.concatenate([own, own, other, other], 0))
            prec[f, :, cols(b)] = 0.5 * (prec[f, :, cols(b)] + back)
        return carry

    lax.fori_loop(0, 2, spread_back, 0)
    for f in range(2):
        store(prec.at[f], prec_hbm.at[f])

    stage_send(1, 1, stage_wait(1, 0))
    stage_send(1, 2, stage_wait(1, 1))
    product = jnp.sum(stage_wait(1, 2), axis=0, keepdims=True)
    rows_ref[0:1, :] = step_row
    rows_ref[1:2, :] = product / rp_row
    rows_ref[2:3, :] = product
    for copy in sent:
        copy.wait_send()
    for copy in outs:
        copy.wait()


def finish(
    sol_hbm, dir_hbm, nr_hbm, prec_hbm, rows, nsol_hbm, nres_hbm, ndir_hbm, nprod_ref, sol, dirn, nr, prec, lsem, osem
):
    def face(ref, f):
        return ref.at[0, :, pl.ds(f * FACE, FACE)]

    loads = [
        [
            pltpu.make_async_copy(src, dst, lsem.at[f, k])
            for k, (src, dst) in enumerate(
                (
                    (nr_hbm.at[f], nr.at[f]),
                    (face(sol_hbm, f), sol.at[f]),
                    (face(dir_hbm, f), dirn.at[f]),
                    (prec_hbm.at[f], prec.at[f]),
                )
            )
        ]
        for f in range(2)
    ]
    for copy in loads[0] + loads[1]:
        copy.start()
    step = jnp.transpose(jnp.broadcast_to(rows[0:1, :], (W, W)))
    ratio = jnp.transpose(jnp.broadcast_to(rows[1:2, :], (W, W)))
    nprod_ref[...] = rows[2:3, :]
    outs = []

    def store(src, dst):
        copy = pltpu.make_async_copy(src, dst, osem.at[len(outs)])
        copy.start()
        outs.append(copy)

    for f in range(2):
        loads[f][0].wait()
        store(nr.at[f], face(nres_hbm, f))
        loads[f][1].wait()
        loads[f][2].wait()
        for b in range(FB):
            sol[f, :, cols(b)] += step * dirn[f, :, cols(b)]
        store(sol.at[f], face(nsol_hbm, f))
        loads[f][3].wait()
        for b in range(FB):
            prec[f, :, cols(b)] += ratio * dirn[f, :, cols(b)]
        store(prec.at[f], face(ndir_hbm, f))
    for copy in outs:
        copy.wait()


def shards(
    solution,
    residual,
    direction,
    residual_product,
    neighbor_slots,
    coupling,
    dirichlet_factor,
    face_block,
    neumann_factor,
    primal_block,
    primal_basis,
    coarse_matrix,
    coarse_block_inverse,
    coarse_pattern,
):
    hbm = pl.BlockSpec(memory_space=pl.ANY)
    vmem = pl.BlockSpec(memory_space=pltpu.VMEM)
    smem = pl.BlockSpec(memory_space=pltpu.SMEM)
    dma = pltpu.SemaphoreType.DMA
    big = jax.ShapeDtypeStruct((1, W, 2 * FACE), F32)
    pair = jax.ShapeDtypeStruct((2, W, FACE), F32)
    nr, prec, rows = pl.pallas_call(
        kernel,
        out_shape=(pair, pair, jax.ShapeDtypeStruct((8, W), F32)),
        in_specs=[hbm, hbm, vmem, smem, hbm, hbm, hbm, hbm, vmem, hbm, hbm, hbm, smem],
        out_specs=(hbm, hbm, vmem),
        scratch_shapes=[
            pltpu.VMEM((96, 2 * W, W), BF16),
            pltpu.VMEM((96, W, W), BF16),
            pltpu.VMEM((32, W, W), BF16),
            pltpu.VMEM((32, W, W), BF16),
            pltpu.VMEM((W, W), BF16),
            pltpu.VMEM((9, W, W), F32),
            pltpu.VMEM((W, W), F32),
            pltpu.VMEM((2, W, FACE), F32),
            pltpu.VMEM((4, W, FACE), F32),
            pltpu.VMEM((4, 2 * W, FACE), BF16),
            pltpu.VMEM((4, W, FACE), F32),
            pltpu.VMEM((4, W, 3 * W), F32),
            pltpu.VMEM((4, W, 3 * W), F32),
            pltpu.VMEM((2, W, FACE), F32),
            pltpu.VMEM((2, W, FACE), F32),
            pltpu.VMEM((2, W, FACE), F32),
            pltpu.VMEM((2, FB, W, W), F32),
            pltpu.VMEM((2, FB, W, W), F32),
            pltpu.VMEM((4, W + 8, W), F32),
            pltpu.VMEM((4, W + 8, W), F32),
            pltpu.VMEM((4, W, W), F32),
            pltpu.VMEM((W, W), F32),
            pltpu.VMEM((2, W, W), F32),
            pltpu.VMEM((2, W, W), F32),
            pltpu.VMEM((4, W, W), F32),
            pltpu.VMEM((4, W, W), F32),
            pltpu.VMEM((2, W, W), F32),
            pltpu.VMEM((2 * REACH + 1, N_GRP, W, W), F32),
            pltpu.VMEM((W, W), F32),
            pltpu.VMEM((2, W, W), F32),
            pltpu.VMEM((W, W), F32),
            pltpu.VMEM((1, W, W), F32),
            pltpu.VMEM((W, W), F32),
            pltpu.VMEM((2, N_GRP, 8, W), F32),
            pltpu.VMEM((2, ROW, 8, W), F32),
            pltpu.VMEM((2, N_X, 8, W), F32),
            dma((11,)),
            dma((4,)),
            dma((3,)), dma((3,)),
            dma((2,)), dma((2,)),
            dma((4,)), dma((4,)),
            dma((2,)), dma((2,)),
            dma((4,)), dma((4,)),
            dma((2, 4)), dma((2, 4)),
            dma((3,)), dma((N_GRP, 4)), dma((2 * REACH + 1, N_GRP)),
            dma((2,)), dma((2,)),
            dma((2, 3)), dma((2, N_GRP)),
            dma((2, 7)), dma((2, ROW)),
            dma((2, 3)), dma((2, N_X)),
        ],
        compiler_params=pltpu.CompilerParams(
            collective_id=0, has_side_effects=True, vmem_limit_bytes=60 * 1024 * 1024
        ),
        name="pcg_step",
    )(
        residual,
        direction,
        residual_product.reshape(1, W),
        neighbor_slots,
        coupling,
        dirichlet_factor,
        face_block,
        neumann_factor,
        primal_block,
        primal_basis,
        coarse_matrix,
        coarse_block_inverse,
        coarse_pattern,
    )
    nsol, nres, ndir, nprod = pl.pallas_call(
        finish,
        out_shape=(big, big, big, jax.ShapeDtypeStruct((1, W), F32)),
        in_specs=[hbm, hbm, hbm, hbm, vmem],
        out_specs=(hbm, hbm, hbm, vmem),
        scratch_shapes=[
            pltpu.VMEM((2, W, FACE), F32),
            pltpu.VMEM((2, W, FACE), F32),
            pltpu.VMEM((2, W, FACE), F32),
            pltpu.VMEM((2, W, FACE), F32),
            dma((2, 4)),
            dma((6,)),
        ],
        name="finish",
    )(solution, direction, nr, prec, rows)
    return nsol, nres, ndir, nprod.reshape(W)


def solution(mesh):
    both = ("sub", "grp")

    def split_first(rank):
        return P(both, *([None] * (rank - 1)))

    return jax.shard_map(
        shards,
        mesh=mesh,
        in_specs=(
            split_first(3), split_first(3), split_first(3), P(), split_first(2), split_first(4), split_first(4),
            split_first(4), split_first(4), split_first(2), split_first(3), split_first(4), split_first(3),
            split_first(2),
        ),
        out_specs=(split_first(3), split_first(3), split_first(3), P()),
        check_vma=False,
    )
```

```python
import functools

import jax
import jax.numpy as jnp
from jax import lax
from jax.experimental import pallas as pl
from jax.experimental.pallas import tpu as pltpu
from jax.sharding import PartitionSpec as P

F32 = jnp.float32
BF16 = jnp.bfloat16
MESH = pl.DeviceIdType.MESH

N_SUB = 32
N_GRP = 4
ROW = 8
N_X = N_SUB // ROW
W = 128
FB = 8
FACE = FB * W
REACH = 2


def split(x):
    hi = x.astype(BF16)
    lo = (x - hi.astype(F32)).astype(BF16)
    return hi, lo


def wide(x):
    return jnp.concatenate(split(x), 1)


def mm(x, w):
    return lax.dot_general(x, w, (((1,), (0,)), ((), ())), preferred_element_type=F32)


def mmt(x, w):
    return lax.dot_general(x, w, (((1,), (1,)), ((), ())), preferred_element_type=F32)


def mm3(x, w):
    xh, xl = split(x)
    wh, wl = split(w)
    return mm(jnp.concatenate([xh, xl], 1), jnp.concatenate([wh, wh], 0)) + mm(xh, wl)


def cols(b):
    return pl.ds(b * W, W)


def kernel(
    res_hbm, dir_hbm, rp_ref, slots, coup_hbm, diri_hbm, face_hbm, neum_hbm, pblk_ref, basis_hbm, cmat_hbm,
    cinv_hbm, patt,
    nr_hbm, prec_hbm, rows_ref,
    coup, diri, face, neum, basis, cmat, cinv, res,
    uf, uhl, yy, tt, ss, c2, nr, prec, nst, nf, bms, bmr, nrel, pbm, crs, crr, cis, cir, ownc, win, cors, corr_in,
    avec, z2, ar_y, ar_z, ar_x,
    lsem, osem, dsend, drecv, nsend, nrecv, bsend, brecv, crsend, crrecv, cisend, cirecv, c2send, c2recv,
    wysend, wssend, wrecv, cosend, corecv, ysend, yrecv, zsend, zrecv, xsend, xrecv,
):
    i = lax.axis_index("sub")
    g = lax.axis_index("grp")
    row = i // ROW
    col = i % ROW

    def at_sub(k):
        return lax.rem(i + k + N_SUB, N_SUB)

    def at_grp(k):
        return lax.rem(g + k + N_GRP, N_GRP)

    def dev(s, t):
        return {"sub": s, "grp": t}

    neighbor = [dev(at_sub(-1), g), dev(at_sub(1), g), dev(i, at_grp(-1)), dev(i, at_grp(1))]
    y_peers = [dev(i, at_grp(k)) for k in range(1, N_GRP)]
    z_peers = [dev(row * ROW + lax.rem(col + k, ROW), g) for k in range(1, ROW)]
    x_peers = [dev(lax.rem(row + k, N_X) * ROW + col, g) for k in range(1, N_X)]
    reach = [k for k in range(-REACH, REACH + 1) if k != 0]
    s_peers = [dev(at_sub(k), g) for k in reach]
    odd = lax.rem(i, 2)
    far = [dev(at_sub(REACH), g), dev(at_sub(-REACH), g)]
    partner = dev(i + 1 - 2 * odd, g)

    local = []

    def load(src, dst):
        copy = pltpu.make_async_copy(src, dst, lsem.at[len(local)])
        copy.start()
        local.append(copy)
        return copy

    l_neum = load(neum_hbm.at[0], neum)
    l_basis = load(basis_hbm.at[0], basis)
    l_dir = [load(dir_hbm.at[0, :, pl.ds(f * FACE, FACE)], uf.at[2 * f + 1]) for f in range(2)]
    l_res = [load(res_hbm.at[0, :, pl.ds(f * FACE, FACE)], res.at[f]) for f in range(2)]
    l_face = load(face_hbm.at[0], face)
    l_coup = load(coup_hbm.at[0], coup)
    l_diri = load(diri_hbm.at[0], diri)
    l_cinv = load(cinv_hbm.at[0], cinv)
    l_cmat = load(cmat_hbm.at[0], cmat)

    barrier = pltpu.get_barrier_semaphore()
    everyone = y_peers + z_peers + x_peers + s_peers
    for peer in everyone:
        pl.semaphore_signal(barrier, inc=1, device_id=peer, device_id_type=MESH)
    pl.semaphore_wait(barrier, len(everyone))

    sent = []

    def send(src, dst, send_sem, recv_sem, peer):
        copy = pltpu.make_async_remote_copy(
            src_ref=src, dst_ref=dst, send_sem=send_sem, recv_sem=recv_sem, device_id=peer, device_id_type=MESH
        )
        copy.start()
        sent.append(copy)

    def arrived(ref, send_sem, recv_sem):
        pltpu.make_async_remote_copy(
            src_ref=ref, dst_ref=ref, send_sem=send_sem, recv_sem=recv_sem, device_id=neighbor[0], device_id_type=MESH
        ).wait_recv()

    half = FACE // 2

    def send_half(h):
        send(
            dir_hbm.at[0, :, pl.ds(FACE + h * half, half)], uf.at[2, :, pl.ds(h * half, half)],
            dsend.at[h], drecv.at[h], neighbor[3],
        )

    send_half(0)
    send(dir_hbm.at[0, :, pl.ds(0, FACE)], uf.at[0], dsend.at[2], drecv.at[2], neighbor[1])

    l_basis.wait()
    pb_row = pblk_ref[...].astype(F32)
    pbm[...] = jnp.transpose(jnp.broadcast_to(pb_row, (W, W)))
    basis_f = basis[...].astype(F32)
    for d in range(4):
        bms[d, 0:W, :] = basis_f
        bms[d, W : W + 8, :] = jnp.broadcast_to(pb_row - (slots[0, d] * FB).astype(F32), (8, W))

    def send_basis(d):
        send(bms.at[d], bmr.at[d ^ 1], bsend.at[d], brecv.at[d ^ 1], neighbor[d])

    def basis_arrived(d):
        arrived(bmr.at[d], bsend.at[d], brecv.at[d])
        nrel[d] = jnp.transpose(jnp.broadcast_to(bmr[d, W : W + 1, :], (W, W)))

    send_basis(2)
    send_basis(0)
    l_neum.wait()
    for f in (1, 0):
        start = slots[0, 2 * f] * FB

        def to_f32(b, carry, f=f, start=start):
            nst[f, b] = neum[start + b].astype(F32)
            return carry

        lax.fori_loop(0, FB, to_f32, 0)
        send(nst.at[f], nf.at[f], nsend.at[f], nrecv.at[f], neighbor[2 * f])
    def own_mask(d, b):
        number = (slots[0, d] * FB + b).astype(F32)
        return jnp.where(pbm[...] == number, basis[...].astype(F32), 0.0).astype(BF16)

    def nb_mask(d, b):
        return jnp.where(nrel[d] == float(b), bmr[d, 0:W, :], 0.0).astype(BF16)

    def coarse_pair(read, d):
        total = None
        for b in range(FB):
            both = jnp.concatenate([own_mask(d, b), nb_mask(d, b)], 0)
            part = mmt(wide(read(b)), jnp.concatenate([both, both], 1))
            total = part if total is None else total + part
        return total

    for copy in l_dir:
        copy.wait()
    l_face.wait()
    l_coup.wait()
    l_diri.wait()

    def interior(jobs):
        first = []
        for lhs, n in jobs:
            two = mm(lhs, coup[n])
            first.append(wide(two[:W] + two[W:]))
        second = []
        for x, (_, n) in zip(first, jobs):
            m = diri[n]
            second.append(wide(mm(x, jnp.concatenate([m, m], 0))))
        third = []
        for x, (_, n) in zip(second, jobs):
            m = diri[n]
            third.append(wide(mmt(x, jnp.concatenate([m, m], 1))))
        out = []
        for x, (_, n) in zip(third, jobs):
            m = coup[n]
            out.append(mmt(x, jnp.concatenate([m, m], 1)))
        return out

    def face_term(d, blocks):
        base = slots[0, d] * FB
        for b in blocks:
            hi, lo = split(uf[d, :, cols(b)])
            uhl[d, 0:W, cols(b)] = hi
            uhl[d, W : 2 * W, cols(b)] = lo
            m = face[base + b]
            yy[d, :, cols(b)] = mm(jnp.concatenate([hi, lo], 1), jnp.concatenate([m, m], 0))

    def within(d, pairs):
        base = slots[0, d] * FB
        for k in range(0, len(pairs), 6):
            group = pairs[k : k + 6]
            jobs = [
                (
                    jnp.concatenate([uhl[d, :, cols(b)], uhl[d, :, cols(b + q + 1)]], 1),
                    q * 4 * FB + base + b,
                )
                for q, b in group
            ]
            for (q, b), out in zip(group, interior(jobs)):
                yy[d, :, cols(b)] += out[:, :W]
                yy[d, :, cols(b + q + 1)] += out[:, W:]

    inside = [(q, b) for q in range(3) for b in range(FB - 1 - q)]
    early = [(q, b) for q, b in inside if b + q + 1 < FB // 2]
    late = [(q, b) for q, b in inside if b + q + 1 >= FB // 2]
    across = [(q, b) for q in range(3) for b in range(FB - 1 - q, FB)]

    def direction_of(slot):
        where = jnp.int32(0)
        for d in range(1, 4):
            where = jnp.where(slots[0, d] == slot, jnp.int32(d), where)
        return where

    def straddling(p, carry):
        slot = lax.rem(slots[0, 2] + 1 + p, 4)
        this = direction_of(slot)
        after = direction_of(lax.rem(slot + 1, 4))
        jobs = [
            (
                jnp.concatenate([uhl[this, :, cols(b)], uhl[after, :, cols(b + q + 1 - FB)]], 1),
                q * 4 * FB + slot * FB + b,
            )
            for q, b in across
        ]
        heads, tails = [None] * 3, [None] * 3
        for (q, b), out in zip(across, interior(jobs)):
            h, m = b - FB + 3, b + q + 1 - FB
            heads[h] = out[:, :W] if heads[h] is None else heads[h] + out[:, :W]
            tails[m] = out[:, W:] if tails[m] is None else tails[m] + out[:, W:]
        for m in range(3):
            tt[p, :, cols(m)] = heads[m]
            ss[p, :, cols(m)] = tails[m]
        return carry

    def return_piece(f, k):
        piece = cols(k)
        send(
            yy.at[2 * f, :, piece], c2.at[f, :, piece], c2send.at[f, k], c2recv.at[f, k], neighbor[2 * f]
        )

    def returned(f):
        for k in range(FB):
            piece = cols(k)
            arrived(c2.at[f, :, piece], c2send.at[f, k], c2recv.at[f, k])

    def first_step(v, value):
        ownc[v] = value
        win[v, REACH, g] = mm3(value, cinv[...])
        for k, peer in enumerate(y_peers):
            send(win.at[v, REACH, g], win.at[v, REACH, g], wysend.at[v, k], wrecv.at[v, REACH, g], peer)
        forward(v, 0)

    def forward(v, k):
        piece = at_grp(k)
        for n, (place, peer) in enumerate(zip((0, 2 * REACH, 1 + 2 * odd), far + [partner])):
            send(win.at[v, REACH, piece], win.at[v, place, piece], wssend.at[v, k, n], wrecv.at[v, place, piece], peer)

    def gathered(v):
        for k in range(1, N_GRP):
            piece = at_grp(k)
            arrived(win.at[v, REACH, piece], wysend.at[v, 0], wrecv.at[v, REACH, piece])
            forward(v, k)

    def relay(v, k):
        piece = at_grp(k)
        place, there = 2 * REACH * (1 - odd), 3 - 2 * odd
        arrived(win.at[v, place, piece], wssend.at[v, 0, 0], wrecv.at[v, place, piece])
        send(win.at[v, place, piece], win.at[v, there, piece], wssend.at[v, k, 3], wrecv.at[v, there, piece], partner)

    def complete(v):
        for k in range(N_GRP):
            piece = at_grp(k)
            for place in (2 * REACH * odd, 1, 3):
                arrived(win.at[v, place, piece], wssend.at[v, 0, 0], wrecv.at[v, place, piece])

    face_term(3, range(FB))
    within(3, inside)
    basis_arrived(3)
    basis_arrived(1)
    for copy in l_res:
        copy.wait()
    ownc[...] = jnp.zeros_like(ownc)

    def coarse_of_residual(f, carry):
        pair = coarse_pair(lambda b: res[f, :, cols(b)], 2 * f + 1)
        ownc[0] += pair[:, :W]
        crs[f] = pair[:, W:]
        return carry

    lax.fori_loop(0, 2, coarse_of_residual, 0)
    for f in range(2):
        send(crs.at[f], crr.at[f], crsend.at[f], crrecv.at[f], neighbor[2 * f + 1])
    send_half(1)
    send_basis(3)
    send_basis(1)

    face_term(1, range(FB))
    within(1, inside)

    arrived(uf.at[2, :, pl.ds(0, half)], dsend.at[0], drecv.at[0])
    face_term(2, range(FB // 2))
    within(2, early)
    for f in range(2):
        arrived(crr.at[f], crsend.at[f], crrecv.at[f])
    l_cinv.wait()
    first_step(0, ownc[0] + (crr[0] + crr[1]))
    arrived(uf.at[0], dsend.at[2], drecv.at[2])
    face_term(0, range(FB))
    within(0, inside)
    lax.fori_loop(0, 3, straddling, 0)
    place = lax.rem(slots[0, 0] - slots[0, 2] + 7, 4)
    for m in range(3):
        yy[0, :, cols(FB - 3 + m)] += tt[place, :, cols(m)]
    for k in range(3, FB):
        return_piece(0, k)
    arrived(uf.at[2, :, pl.ds(half, half)], dsend.at[1], drecv.at[1])
    face_term(2, range(FB // 2, FB))
    within(2, late)
    for m in range(3):
        yy[2, :, cols(m)] += ss[2, :, cols(m)]
    return_piece(1, 0)
    straddling(3, 0)
    for d in range(4):
        place = lax.rem(slots[0, d] - slots[0, 2] + 7, 4)
        before = lax.rem(slots[0, d] - slots[0, 2] + 6, 4)
        for m in range(3):
            if d != 2:
                yy[d, :, cols(m)] += ss[before, :, cols(m)]
            if d != 0:
                yy[d, :, cols(FB - 3 + m)] += tt[place, :, cols(m)]

    def folded(x):
        return jnp.sum(jnp.transpose(x).reshape(W // 8, 8, W), axis=0)

    stages = (
        (ar_y, ysend, yrecv, N_GRP, g, y_peers),
        (ar_z, zsend, zrecv, ROW, col, z_peers),
        (ar_x, xsend, xrecv, N_X, row, x_peers),
    )

    def stage_send(which, stage, value):
        buf, ssem, rsem, count, me, peers = stages[stage]
        buf[which, me] = value
        for k, peer in enumerate(peers):
            send(buf.at[which, me], buf.at[which, me], ssem.at[which, k], rsem.at[which, me], peer)

    def stage_wait(which, stage):
        buf, ssem, rsem, count, me, peers = stages[stage]
        for k in range(1, count):
            other = lax.rem(me + k, count)
            arrived(buf.at[which, other], ssem.at[which, 0], rsem.at[which, other])
        total = buf[which, 0]
        for k in range(1, count):
            total = total + buf[which, k]
        return total

    def curve(d, acc):
        for b in range(FB):
            acc = acc + uf[d, :, cols(b)] * yy[d, :, cols(b)]
        return acc

    stage_send(0, 0, folded(lax.fori_loop(0, 4, curve, jnp.zeros((W, W), F32))))

    return_piece(1, 1)
    for k in range(3):
        return_piece(0, k)
    basis_arrived(0)
    basis_arrived(2)

    def coarse_of_image(k, carry):
        d = lax.rem(k + 2, 4)
        pair = coarse_pair(lambda b: yy[d, :, cols(b)], d)
        ownc[1] += pair[:, :W]
        cis[d] = pair[:, W:]
        return carry

    lax.fori_loop(0, 2, coarse_of_image, 0)
    for d in (2, 3):
        send(cis.at[d], cir.at[d ^ 1], cisend.at[d], cirecv.at[d ^ 1], neighbor[d])
    lax.fori_loop(2, 4, coarse_of_image, 0)
    for d in (0, 1):
        send(cis.at[d], cir.at[d ^ 1], cisend.at[d], cirecv.at[d ^ 1], neighbor[d])

    for k in range(2, 5):
        return_piece(1, k)
    stage_send(0, 1, stage_wait(0, 0))
    gathered(0)
    for d in range(4):
        arrived(cir.at[d], cisend.at[d], cirecv.at[d])
    first_step(1, ownc[1] + ((cir[0] + cir[1]) + (cir[2] + cir[3])))
    for k in range(5, FB):
        return_piece(1, k)
    stage_send(0, 2, stage_wait(0, 1))
    gathered(1)
    for k in range(N_GRP):
        relay(0, k)
    rp_row = rp_ref[...]
    curvature = jnp.sum(stage_wait(0, 2), axis=0, keepdims=True)
    step_row = rp_row / curvature
    avec[...] = jnp.transpose(jnp.broadcast_to(step_row, (W, W)))
    relay(1, 0)

    outs = []

    def store(src, dst):
        copy = pltpu.make_async_copy(src, dst, osem.at[len(outs)])
        copy.start()
        outs.append(copy)

    z2[...] = jnp.zeros_like(z2)

    def own_face(f):
        a = avec[...]
        base = slots[0, 2 * f + 1] * FB
        acc = z2[...]
        for b in range(FB):
            new = res[f, :, cols(b)] - a * (yy[2 * f + 1, :, cols(b)] + c2[f, :, cols(b)])
            nr[f, :, cols(b)] = new
            mine = neum[base + b]
            theirs = nf[f, b].astype(BF16)
            both = jnp.concatenate([mine, theirs], 1)
            z = mm(wide(0.5 * new), jnp.concatenate([both, both], 0))
            acc = acc + (z[:, :W] * z[:, :W] + z[:, W:] * z[:, W:])
            lhs = jnp.concatenate([wide(z[:, :W]), wide(z[:, W:])], 1)
            prec[f, :, cols(b)] = mmt(lhs, jnp.concatenate([mine, mine, theirs, theirs], 1))
        z2[...] = acc

    returned(0)
    arrived(nf.at[0], nsend.at[0], nrecv.at[0])
    own_face(0)
    relay(1, 1)
    relay(1, 2)
    returned(1)
    arrived(nf.at[1], nsend.at[1], nrecv.at[1])
    own_face(1)
    for f in range(2):
        store(nr.at[f], nr_hbm.at[f])

    relay(1, 3)
    complete(0)
    complete(1)
    l_cmat.wait()
    a = 0.5 * avec[...]

    def combined(place, piece):
        return 0.5 * win[0, place, piece] - a * win[1, place, piece]

    adjacent = None
    for k in range(9):
        entry = patt[0, k]
        place = jnp.minimum(lax.rem(entry // N_GRP - i + REACH + N_SUB, N_SUB), 2 * REACH)
        part = mm3(combined(place, lax.rem(entry, N_GRP)), cmat[k])
        adjacent = part if adjacent is None else adjacent + part
    coarse_res = 0.5 * ownc[0] - a * ownc[1]
    corr = combined(REACH, g) + mm3(coarse_res - adjacent, cinv[...])
    cors[...] = corr
    stage_send(1, 0, folded(z2[...] + corr * coarse_res))
    for f in (1, 0):
        send(cors, corr_in.at[f], cosend.at[f], corecv.at[f], neighbor[2 * f])
    stage_send(1, 1, stage_wait(1, 0))
    stage_send(1, 2, stage_wait(1, 1))
    for f in range(2):
        arrived(corr_in.at[f], cosend.at[f], corecv.at[f])

    def spread_back(f, carry):
        lhs = jnp.concatenate([wide(cors[...]), wide(corr_in[f])], 1)
        for b in range(FB):
            own = own_mask(2 * f + 1, b)
            other = nb_mask(2 * f + 1, b)
            back = mm(lhs, jnp.concatenate([own, own, other, other], 0))
            prec[f, :, cols(b)] = 0.5 * (prec[f, :, cols(b)] + back)
        return carry

    lax.fori_loop(0, 2, spread_back, 0)
    for f in range(2):
        store(prec.at[f], prec_hbm.at[f])

    product = jnp.sum(stage_wait(1, 2), axis=0, keepdims=True)
    rows_ref[0:1, :] = step_row
    rows_ref[1:2, :] = product / rp_row
    rows_ref[2:3, :] = product
    for copy in sent:
        copy.wait_send()
    for copy in outs:
        copy.wait()


def finish(
    sol_hbm, dir_hbm, nr_hbm, prec_hbm, rows, nsol_hbm, nres_hbm, ndir_hbm, nprod_ref, sol, dirn, nr, prec, lsem, osem
):
    def face(ref, f):
        return ref.at[0, :, pl.ds(f * FACE, FACE)]

    loads = [
        [
            pltpu.make_async_copy(src, dst, lsem.at[f, k])
            for k, (src, dst) in enumerate(
                (
                    (nr_hbm.at[f], nr.at[f]),
                    (face(sol_hbm, f), sol.at[f]),
                    (face(dir_hbm, f), dirn.at[f]),
                    (prec_hbm.at[f], prec.at[f]),
                )
            )
        ]
        for f in range(2)
    ]
    for copy in loads[0] + loads[1]:
        copy.start()
    step = jnp.transpose(jnp.broadcast_to(rows[0:1, :], (W, W)))
    ratio = jnp.transpose(jnp.broadcast_to(rows[1:2, :], (W, W)))
    nprod_ref[...] = rows[2:3, :]
    outs = []

    def store(src, dst):
        copy = pltpu.make_async_copy(src, dst, osem.at[len(outs)])
        copy.start()
        outs.append(copy)

    for f in range(2):
        loads[f][0].wait()
        store(nr.at[f], face(nres_hbm, f))
        loads[f][1].wait()
        loads[f][2].wait()
        for b in range(FB):
            sol[f, :, cols(b)] += step * dirn[f, :, cols(b)]
        store(sol.at[f], face(nsol_hbm, f))
        loads[f][3].wait()
        for b in range(FB):
            prec[f, :, cols(b)] += ratio * dirn[f, :, cols(b)]
        store(prec.at[f], face(ndir_hbm, f))
    for copy in outs:
        copy.wait()


def shards(
    solution,
    residual,
    direction,
    residual_product,
    neighbor_slots,
    coupling,
    dirichlet_factor,
    face_block,
    neumann_factor,
    primal_block,
    primal_basis,
    coarse_matrix,
    coarse_block_inverse,
    coarse_pattern,
):
    hbm = pl.BlockSpec(memory_space=pl.ANY)
    vmem = pl.BlockSpec(memory_space=pltpu.VMEM)
    smem = pl.BlockSpec(memory_space=pltpu.SMEM)
    dma = pltpu.SemaphoreType.DMA
    big = jax.ShapeDtypeStruct((1, W, 2 * FACE), F32)
    pair = jax.ShapeDtypeStruct((2, W, FACE), F32)
    nr, prec, rows = pl.pallas_call(
        kernel,
        out_shape=(pair, pair, jax.ShapeDtypeStruct((8, W), F32)),
        in_specs=[hbm, hbm, vmem, smem, hbm, hbm, hbm, hbm, vmem, hbm, hbm, hbm, smem],
        out_specs=(hbm, hbm, vmem),
        scratch_shapes=[
            pltpu.VMEM((96, 2 * W, W), BF16),
            pltpu.VMEM((96, W, W), BF16),
            pltpu.VMEM((32, W, W), BF16),
            pltpu.VMEM((32, W, W), BF16),
            pltpu.VMEM((W, W), BF16),
            pltpu.VMEM((9, W, W), F32),
            pltpu.VMEM((W, W), F32),
            pltpu.VMEM((2, W, FACE), F32),
            pltpu.VMEM((4, W, FACE), F32),
            pltpu.VMEM((4, 2 * W, FACE), BF16),
            pltpu.VMEM((4, W, FACE), F32),
            pltpu.VMEM((4, W, 3 * W), F32),
            pltpu.VMEM((4, W, 3 * W), F32),
            pltpu.VMEM((2, W, FACE), F32),
            pltpu.VMEM((2, W, FACE), F32),
            pltpu.VMEM((2, W, FACE), F32),
            pltpu.VMEM((2, FB, W, W), F32),
            pltpu.VMEM((2, FB, W, W), F32),
            pltpu.VMEM((4, W + 8, W), F32),
            pltpu.VMEM((4, W + 8, W), F32),
            pltpu.VMEM((4, W, W), F32),
            pltpu.VMEM((W, W), F32),
            pltpu.VMEM((2, W, W), F32),
            pltpu.VMEM((2, W, W), F32),
            pltpu.VMEM((4, W, W), F32),
            pltpu.VMEM((4, W, W), F32),
            pltpu.VMEM((2, W, W), F32),
            pltpu.VMEM((2, 2 * REACH + 1, N_GRP, W, W), F32),
            pltpu.VMEM((W, W), F32),
            pltpu.VMEM((2, W, W), F32),
            pltpu.VMEM((W, W), F32),
            pltpu.VMEM((W, W), F32),
            pltpu.VMEM((2, N_GRP, 8, W), F32),
            pltpu.VMEM((2, ROW, 8, W), F32),
            pltpu.VMEM((2, N_X, 8, W), F32),
            dma((11,)),
            dma((4,)),
            dma((3,)), dma((3,)),
            dma((2,)), dma((2,)),
            dma((4,)), dma((4,)),
            dma((2,)), dma((2,)),
            dma((4,)), dma((4,)),
            dma((2, FB)), dma((2, FB)),
            dma((2, 3)), dma((2, N_GRP, 4)), dma((2, 2 * REACH + 1, N_GRP)),
            dma((2,)), dma((2,)),
            dma((2, 3)), dma((2, N_GRP)),
            dma((2, 7)), dma((2, ROW)),
            dma((2, 3)), dma((2, N_X)),
        ],
        compiler_params=pltpu.CompilerParams(
            collective_id=0, has_side_effects=True, vmem_limit_bytes=60 * 1024 * 1024
        ),
        name="pcg_step",
    )(
        residual,
        direction,
        residual_product.reshape(1, W),
        neighbor_slots,
        coupling,
        dirichlet_factor,
        face_block,
        neumann_factor,
        primal_block,
        primal_basis,
        coarse_matrix,
        coarse_block_inverse,
        coarse_pattern,
    )
    nsol, nres, ndir, nprod = pl.pallas_call(
        finish,
        out_shape=(big, big, big, jax.ShapeDtypeStruct((1, W), F32)),
        in_specs=[hbm, hbm, hbm, hbm, vmem],
        out_specs=(hbm, hbm, hbm, vmem),
        scratch_shapes=[
            pltpu.VMEM((2, W, FACE), F32),
            pltpu.VMEM((2, W, FACE), F32),
            pltpu.VMEM((2, W, FACE), F32),
            pltpu.VMEM((2, W, FACE), F32),
            dma((2, 4)),
            dma((6,)),
        ],
        name="finish",
    )(solution, direction, nr, prec, rows)
    return nsol, nres, ndir, nprod.reshape(W)


def solution(mesh):
    both = ("sub", "grp")

    def split_first(rank):
        return P(both, *([None] * (rank - 1)))

    return jax.shard_map(
        shards,
        mesh=mesh,
        in_specs=(
            split_first(3), split_first(3), split_first(3), P(), split_first(2), split_first(4), split_first(4),
            split_first(4), split_first(4), split_first(2), split_first(3), split_first(4), split_first(3),
            split_first(2),
        ),
        out_specs=(split_first(3), split_first(3), split_first(3), P()),
        check_vma=False,
    )
```

```python
import functools

import jax
import jax.numpy as jnp
from jax import lax
from jax.experimental import pallas as pl
from jax.experimental.pallas import tpu as pltpu
from jax.sharding import PartitionSpec as P

F32 = jnp.float32
BF16 = jnp.bfloat16
MESH = pl.DeviceIdType.MESH

N_SUB = 32
N_GRP = 4
ROW = 8
N_X = N_SUB // ROW
W = 128
FB = 8
FACE = FB * W
REACH = 2


def split(x):
    hi = x.astype(BF16)
    lo = (x - hi.astype(F32)).astype(BF16)
    return hi, lo


def wide(x):
    return jnp.concatenate(split(x), 1)


def mm(x, w):
    return lax.dot_general(x, w, (((1,), (0,)), ((), ())), preferred_element_type=F32)


def mmt(x, w):
    return lax.dot_general(x, w, (((1,), (1,)), ((), ())), preferred_element_type=F32)


def mm3(x, w):
    xh, xl = split(x)
    wh, wl = split(w)
    return mm(jnp.concatenate([xh, xl], 1), jnp.concatenate([wh, wh], 0)) + mm(xh, wl)


def cols(b):
    return pl.ds(b * W, W)


def kernel(
    res_hbm, dir_hbm, rp_ref, slots, coup_hbm, diri_hbm, face_hbm, neum_hbm, pblk_ref, basis_hbm, cmat_hbm,
    cinv_hbm, patt,
    nr_hbm, prec_hbm, rows_ref,
    coup0, coup1, coup2, diri0, diri1, diri2, face, neum, basis, cmat, cinv, res,
    uf, uhl, yy, tt, ss, c2, nr, prec, nst, nf, bms, bmr, masks, crs, crr, cis, cir, ownc, steps, win, cors, corr_in,
    avec, z2, ar_p, ar_z,
    lsem, osem, dsend, drecv, nsend, nrecv, bsend, brecv, crsend, crrecv, cisend, cirecv, c2send, c2recv,
    wysend, wyrecv, wssend, wrecv, cosend, corecv, psend, precv, zsend, zrecv,
):
    i = lax.axis_index("sub")
    g = lax.axis_index("grp")
    row = i // ROW
    col = i % ROW

    def at_sub(k):
        return lax.rem(i + k + N_SUB, N_SUB)

    def at_grp(k):
        return lax.rem(g + k + N_GRP, N_GRP)

    def dev(s, t):
        return {"sub": s, "grp": t}

    neighbor = [dev(at_sub(-1), g), dev(at_sub(1), g), dev(i, at_grp(-1)), dev(i, at_grp(1))]
    y_peers = [dev(i, at_grp(k)) for k in range(1, N_GRP)]
    z_peers = [dev(row * ROW + lax.rem(col + k, ROW), g) for k in range(1, ROW)]
    plane = row * N_GRP + g
    many_plane = N_X * N_GRP

    def in_plane(k):
        other = lax.rem(plane + k, many_plane)
        return dev(other // N_GRP * ROW + col, lax.rem(other, N_GRP))

    p_peers = [in_plane(k) for k in range(1, many_plane)]
    reach = [k for k in range(-REACH, REACH + 1) if k != 0]
    s_peers = [dev(at_sub(k), g) for k in reach]
    odd = lax.rem(i, 2)
    far = [dev(at_sub(REACH), g), dev(at_sub(-REACH), g)]
    partner = dev(i + 1 - 2 * odd, g)

    local = []

    def load(src, dst):
        copy = pltpu.make_async_copy(src, dst, lsem.at[len(local)])
        copy.start()
        local.append(copy)
        return copy

    coup = (coup0, coup1, coup2)
    diri = (diri0, diri1, diri2)
    many = 4 * FB
    l_basis = load(basis_hbm.at[0], basis)
    l_dir = [load(dir_hbm.at[0, :, pl.ds(f * FACE, FACE)], uf.at[2 * f + 1]) for f in (1, 0)]
    l_face = load(face_hbm.at[0], face)
    l_interior = []
    for q in range(3):
        if q == 1:
            l_neum = load(neum_hbm.at[0], neum)
        l_interior.append(
            (
                load(coup_hbm.at[0, pl.ds(q * many, many)], coup[q]),
                load(diri_hbm.at[0, pl.ds(q * many, many)], diri[q]),
            )
        )
    l_res = [load(res_hbm.at[0, :, pl.ds(f * FACE, FACE)], res.at[f]) for f in range(2)]
    l_cinv = load(cinv_hbm.at[0], cinv)
    l_cmat = load(cmat_hbm.at[0], cmat)

    barrier = pltpu.get_barrier_semaphore()
    everyone = p_peers + z_peers + s_peers
    for peer in everyone:
        pl.semaphore_signal(barrier, inc=1, device_id=peer, device_id_type=MESH)
    pl.semaphore_wait(barrier, len(everyone))

    sent = []

    def send(src, dst, send_sem, recv_sem, peer):
        copy = pltpu.make_async_remote_copy(
            src_ref=src, dst_ref=dst, send_sem=send_sem, recv_sem=recv_sem, device_id=peer, device_id_type=MESH
        )
        copy.start()
        sent.append(copy)

    def arrived(ref, send_sem, recv_sem):
        pltpu.make_async_remote_copy(
            src_ref=ref, dst_ref=ref, send_sem=send_sem, recv_sem=recv_sem, device_id=neighbor[0], device_id_type=MESH
        ).wait_recv()

    chunks = ((0, 4), (4, 6), (6, FB))

    def chunk(h):
        return pl.ds(chunks[h][0] * W, (chunks[h][1] - chunks[h][0]) * W)

    for h, (start, stop) in enumerate(chunks):
        send(
            dir_hbm.at[0, :, pl.ds(FACE + start * W, (stop - start) * W)], uf.at[2, :, chunk(h)],
            dsend.at[h], drecv.at[h], neighbor[3],
        )
    send(dir_hbm.at[0, :, pl.ds(0, FACE)], uf.at[0], dsend.at[3], drecv.at[3], neighbor[1])

    l_basis.wait()
    pb_row = pblk_ref[...].astype(F32)
    basis_t = jnp.transpose(basis[...].astype(F32))
    for d in range(4):
        bms[d, 0:W, :] = basis_t
        bms[d, W : W + 8, :] = jnp.broadcast_to(pb_row - (slots[0, d] * FB).astype(F32), (8, W))

    def send_basis(d):
        send(bms.at[d], bmr.at[d ^ 1], bsend.at[d], brecv.at[d ^ 1], neighbor[d])

    def basis_arrived(d):
        arrived(bmr.at[d], bsend.at[d], brecv.at[d])
        nb_masks(d)

    for d in (2, 0, 3, 1):
        send_basis(d)
    def own_masks(d, carry):
        for b in range(FB):
            number = (slots[0, d] * FB + b).astype(F32)
            masks[d, b, :, 0:W] = jnp.where(pb_row == number, bms[0, 0:W, :], 0.0).astype(BF16)
        return carry

    lax.fori_loop(0, 4, own_masks, 0)

    def nb_masks(d):
        rel = bmr[d, W : W + 1, :]
        for b in range(FB):
            masks[d, b, :, W : 2 * W] = jnp.where(rel == float(b), bmr[d, 0:W, :], 0.0).astype(BF16)

    def coarse_pair(read, d):
        sums = [None, None]
        for b in range(FB):
            both = masks[d, b]
            part = mm(wide(read(b)), jnp.concatenate([both, both], 0))
            sums[b % 2] = part if sums[b % 2] is None else sums[b % 2] + part
        return sums[0] + sums[1]

    l_dir[0].wait()
    l_face.wait()
    for copy in l_interior[0]:
        copy.wait()

    def chain(jobs):
        first = []
        for (hi, lo), n in jobs:
            m = coup[n[0]][n[1]]
            first.append(wide(mm(jnp.concatenate([hi, lo], 1), jnp.concatenate([m, m], 0))))
        second = []
        for x, (_, n) in zip(first, jobs):
            m = diri[n[0]][n[1]]
            second.append(wide(mm(x, jnp.concatenate([m, m], 0))))
        third = []
        for x, (_, n) in zip(second, jobs):
            m = diri[n[0]][n[1]]
            third.append(wide(mmt(x, jnp.concatenate([m, m], 1))))
        out = []
        for x, (_, n) in zip(third, jobs):
            m = coup[n[0]][n[1]]
            out.append(mmt(x, jnp.concatenate([m, m], 1)))
        return out

    def interior(jobs, size=9):
        out = []
        for k in range(0, len(jobs), size):
            out += chain(jobs[k : k + size])
        return out

    def pair_of(d, b, e, c):
        hi = jnp.concatenate([uhl[d, 0:W, cols(b)], uhl[e, 0:W, cols(c)]], 1)
        lo = jnp.concatenate([uhl[d, W : 2 * W, cols(b)], uhl[e, W : 2 * W, cols(c)]], 1)
        return hi, lo

    def face_term(d, blocks):
        base = slots[0, d] * FB
        for b in blocks:
            hi, lo = split(uf[d, :, cols(b)])
            uhl[d, 0:W, cols(b)] = hi
            uhl[d, W : 2 * W, cols(b)] = lo
            m = face[base + b]
            yy[d, :, cols(b)] = mm(jnp.concatenate([hi, lo], 1), jnp.concatenate([m, m], 0))

    def within_jobs(d, pairs):
        base = slots[0, d] * FB
        return [(pair_of(d, b, d, b + q + 1), (q, base + b)) for q, b in pairs]

    def within_sink(d, pairs, outs):
        for (q, b), out in zip(pairs, outs):
            yy[d, :, cols(b)] += out[:, :W]
            yy[d, :, cols(b + q + 1)] += out[:, W:]

    def within(d, pairs):
        within_sink(d, pairs, interior(within_jobs(d, pairs)))

    inside = [(q, b) for q in range(3) for b in range(FB - 1 - q)]
    early, middle, late = [[(q, b) for q, b in inside if start <= b + q + 1 < stop] for start, stop in chunks]
    across = [(q, b) for q in range(3) for b in range(FB - 1 - q, FB)]

    def direction_of(slot):
        where = jnp.int32(0)
        for d in range(1, 4):
            where = jnp.where(slots[0, d] == slot, jnp.int32(d), where)
        return where

    def straddling_jobs(places):
        jobs = []
        for p in places:
            slot = lax.rem(slots[0, 2] + 1 + p, 4)
            this = direction_of(slot)
            after = direction_of(lax.rem(slot + 1, 4))
            for q, b in across:
                jobs.append((pair_of(this, b, after, b + q + 1 - FB), (q, slot * FB + b)))
        return jobs

    def straddling_sink(places, outs):
        sinks = [(p, b - FB + 3, b + q + 1 - FB) for p in places for q, b in across]
        heads, tails = {}, {}
        for (p, h, m), out in zip(sinks, outs):
            heads[p, h] = heads[p, h] + out[:, :W] if (p, h) in heads else out[:, :W]
            tails[p, m] = tails[p, m] + out[:, W:] if (p, m) in tails else out[:, W:]
        for (p, m), value in heads.items():
            tt[p, :, cols(m)] = value
        for (p, m), value in tails.items():
            ss[p, :, cols(m)] = value

    def return_piece(f, k):
        piece = cols(k)
        send(
            yy.at[2 * f, :, piece], c2.at[f, :, piece], c2send.at[f, k], c2recv.at[f, k], neighbor[2 * f]
        )

    def returned(f, blocks):
        for k in blocks:
            piece = cols(k)
            arrived(c2.at[f, :, piece], c2send.at[f, k], c2recv.at[f, k])

    def first_step(v, value):
        ownc[v] = value
        steps[v, g] = mm3(value, cinv[...])
        for k, peer in enumerate(y_peers):
            send(steps.at[v, g], steps.at[v, g], wysend.at[v, k], wyrecv.at[v, g], peer)

    def forward(k):
        piece = at_grp(k)
        if k > 0:
            for v in range(2):
                arrived(steps.at[v, piece], wysend.at[v, 0], wyrecv.at[v, piece])
        win[REACH, piece] = 0.5 * (steps[0, piece] - avec[...] * steps[1, piece])
        for n, (place, peer) in enumerate(zip((0, 2 * REACH, 1 + 2 * odd), far + [partner])):
            send(win.at[REACH, piece], win.at[place, piece], wssend.at[k, n], wrecv.at[place, piece], peer)

    def relay(k):
        piece = at_grp(k)
        place, there = 2 * REACH * (1 - odd), 3 - 2 * odd
        arrived(win.at[place, piece], wssend.at[0, 0], wrecv.at[place, piece])
        send(win.at[place, piece], win.at[there, piece], wssend.at[k, 3], wrecv.at[there, piece], partner)

    def complete():
        for k in range(N_GRP):
            piece = at_grp(k)
            for place in (2 * REACH * odd, 1, 3):
                arrived(win.at[place, piece], wssend.at[0, 0], wrecv.at[place, piece])

    face_term(3, range(FB))
    within(3, [(q, b) for q, b in inside if q == 0])
    for copy in l_interior[1]:
        copy.wait()
    within(3, [(q, b) for q, b in inside if q == 1])
    for copy in l_interior[2]:
        copy.wait()
    within(3, [(q, b) for q, b in inside if q == 2])
    l_neum.wait()
    for f in (1, 0):
        start = slots[0, 2 * f] * FB

        def to_f32(b, carry, f=f, start=start):
            nst[f, b] = neum[start + b].astype(F32)
            return carry

        lax.fori_loop(0, FB, to_f32, 0)
        send(nst.at[f], nf.at[f], nsend.at[f], nrecv.at[f], neighbor[2 * f])

    basis_arrived(3)
    basis_arrived(1)
    for copy in l_res:
        copy.wait()

    pairs = [coarse_pair(lambda b, f=f: res[f, :, cols(b)], 2 * f + 1) for f in range(2)]
    ownc[0] = pairs[0][:, :W] + pairs[1][:, :W]
    for f in range(2):
        crs[f] = pairs[f][:, W:]
    for f in range(2):
        send(crs.at[f], crr.at[f], crsend.at[f], crrecv.at[f], neighbor[2 * f + 1])

    l_dir[1].wait()
    face_term(1, range(FB))
    within(1, inside)

    arrived(uf.at[2, :, chunk(0)], dsend.at[0], drecv.at[0])
    face_term(2, range(*chunks[0]))
    within(2, early)
    arrived(uf.at[0], dsend.at[3], drecv.at[3])
    face_term(0, range(FB))
    within(0, inside)
    straddling_sink((0, 1, 2), interior(straddling_jobs((0, 1, 2))))
    place = lax.rem(slots[0, 0] - slots[0, 2] + 7, 4)
    for m in range(3):
        yy[0, :, cols(FB - 3 + m)] += tt[place, :, cols(m)]
    for k in range(3, FB):
        return_piece(0, k)
    basis_arrived(0)
    arrived(uf.at[2, :, chunk(1)], dsend.at[1], drecv.at[1])
    face_term(2, range(*chunks[1]))
    within(2, middle)
    for m in range(3):
        yy[2, :, cols(m)] += ss[2, :, cols(m)]
    return_piece(1, 0)
    return_piece(1, 1)
    arrived(uf.at[2, :, chunk(2)], dsend.at[2], drecv.at[2])
    face_term(2, range(*chunks[2]))
    outs = interior(within_jobs(2, late) + straddling_jobs((3,)), 6)
    within_sink(2, late, outs[: len(late)])
    straddling_sink((3,), outs[len(late) :])
    for d in range(4):
        place = lax.rem(slots[0, d] - slots[0, 2] + 7, 4)
        before = lax.rem(slots[0, d] - slots[0, 2] + 6, 4)
        for m in range(3):
            if d != 2:
                yy[d, :, cols(m)] += ss[before, :, cols(m)]
            if d != 0:
                yy[d, :, cols(FB - 3 + m)] += tt[place, :, cols(m)]

    def folded(x):
        return jnp.sum(jnp.transpose(x).reshape(W // 8, 8, W), axis=0)

    stages = (
        (ar_p, psend, precv, many_plane, plane, p_peers),
        (ar_z, zsend, zrecv, ROW, col, z_peers),
    )

    def stage_send(which, stage, value):
        buf, ssem, rsem, count, me, peers = stages[stage]
        buf[which, me] = value
        for k, peer in enumerate(peers):
            send(buf.at[which, me], buf.at[which, me], ssem.at[which, k], rsem.at[which, me], peer)

    def stage_wait(which, stage):
        buf, ssem, rsem, count, me, peers = stages[stage]
        for k in range(1, count):
            other = lax.rem(me + k, count)
            arrived(buf.at[which, other], ssem.at[which, 0], rsem.at[which, other])
        total = buf[which, 0]
        for k in range(1, count):
            total = total + buf[which, k]
        return total

    def curve(d, acc):
        for b in range(FB):
            acc = acc + uf[d, :, cols(b)] * yy[d, :, cols(b)]
        return acc

    stage_send(0, 0, folded(lax.fori_loop(0, 4, curve, jnp.zeros((W, W), F32))))

    basis_arrived(2)

    for first in (2, 0):
        pairs = [coarse_pair(lambda b, d=d: yy[d, :, cols(b)], d) for d in (first, first + 1)]
        for d, pair in zip((first, first + 1), pairs):
            cis[d] = pair[:, W:]
            send(cis.at[d], cir.at[d ^ 1], cisend.at[d], cirecv.at[d ^ 1], neighbor[d])
        both = pairs[0][:, :W] + pairs[1][:, :W]
        ownc[1] = both if first == 2 else ownc[1] + both

    for f in range(2):
        arrived(crr.at[f], crsend.at[f], crrecv.at[f])
    l_cinv.wait()
    first_step(0, ownc[0] + (crr[0] + crr[1]))
    stage_send(0, 1, stage_wait(0, 0))
    for k in range(3):
        return_piece(0, k)
    for k in range(2, 3):
        return_piece(1, k)
    for d in range(4):
        arrived(cir.at[d], cisend.at[d], cirecv.at[d])
    first_step(1, ownc[1] + ((cir[0] + cir[1]) + (cir[2] + cir[3])))
    for k in range(3, FB):
        return_piece(1, k)
    rp_row = rp_ref[...]
    curvature = jnp.sum(stage_wait(0, 1), axis=0, keepdims=True)
    step_row = rp_row / curvature
    avec[...] = jnp.transpose(jnp.broadcast_to(step_row, (W, W)))
    forward(0)
    for k in range(1, N_GRP):
        forward(k)
    relay(0)

    outs = []

    def store(src, dst):
        copy = pltpu.make_async_copy(src, dst, osem.at[len(outs)])
        copy.start()
        outs.append(copy)

    z2[...] = jnp.zeros_like(z2)

    def own_face(f, blocks):
        a = avec[...]
        base = slots[0, 2 * f + 1] * FB
        acc = z2[...]
        for b in blocks:
            new = res[f, :, cols(b)] - a * (yy[2 * f + 1, :, cols(b)] + c2[f, :, cols(b)])
            nr[f, :, cols(b)] = new
            mine = neum[base + b]
            theirs = nf[f, b].astype(BF16)
            both = jnp.concatenate([mine, theirs], 1)
            z = mm(wide(0.5 * new), jnp.concatenate([both, both], 0))
            acc = acc + (z[:, :W] * z[:, :W] + z[:, W:] * z[:, W:])
            lhs = jnp.concatenate([wide(z[:, :W]), wide(z[:, W:])], 1)
            prec[f, :, cols(b)] = mmt(lhs, jnp.concatenate([mine, mine, theirs, theirs], 1))
        z2[...] = acc

    returned(0, range(FB))
    arrived(nf.at[0], nsend.at[0], nrecv.at[0])
    own_face(0, range(FB))
    relay(1)
    arrived(nf.at[1], nsend.at[1], nrecv.at[1])
    returned(1, range(4))
    own_face(1, range(4))
    relay(2)
    returned(1, range(4, FB))
    own_face(1, range(4, FB))
    for f in range(2):
        store(nr.at[f], nr_hbm.at[f])

    relay(3)
    complete()
    l_cmat.wait()
    adjacent = None
    for k in range(9):
        entry = patt[0, k]
        place = jnp.minimum(lax.rem(entry // N_GRP - i + REACH + N_SUB, N_SUB), 2 * REACH)
        part = mm3(win[place, lax.rem(entry, N_GRP)], cmat[k])
        adjacent = part if adjacent is None else adjacent + part
    coarse_res = 0.5 * (ownc[0] - avec[...] * ownc[1])
    corr = win[REACH, g] + mm3(coarse_res - adjacent, cinv[...])
    cors[...] = corr
    stage_send(1, 0, folded(z2[...] + corr * coarse_res))
    for f in (1, 0):
        send(cors, corr_in.at[f], cosend.at[f], corecv.at[f], neighbor[2 * f])
    stage_send(1, 1, stage_wait(1, 0))
    for f in range(2):
        arrived(corr_in.at[f], cosend.at[f], corecv.at[f])

    def spread_back(f, carry):
        lhs = jnp.concatenate([wide(cors[...]), wide(corr_in[f])], 1)
        for b in range(FB):
            own = masks[2 * f + 1, b, :, 0:W]
            other = masks[2 * f + 1, b, :, W : 2 * W]
            back = mmt(lhs, jnp.concatenate([own, own, other, other], 1))
            prec[f, :, cols(b)] = 0.5 * (prec[f, :, cols(b)] + back)
        return carry

    lax.fori_loop(0, 2, spread_back, 0)
    for f in range(2):
        store(prec.at[f], prec_hbm.at[f])

    product = jnp.sum(stage_wait(1, 1), axis=0, keepdims=True)
    rows_ref[0:1, :] = step_row
    rows_ref[1:2, :] = product / rp_row
    rows_ref[2:3, :] = product
    for copy in sent:
        copy.wait_send()
    for copy in outs:
        copy.wait()


def finish(
    sol_hbm, dir_hbm, nr_hbm, prec_hbm, rows, nsol_hbm, nres_hbm, ndir_hbm, nprod_ref, sol, dirn, nr, prec, lsem, osem
):
    def face(ref, f):
        return ref.at[0, :, pl.ds(f * FACE, FACE)]

    loads = [
        [
            pltpu.make_async_copy(src, dst, lsem.at[f, k])
            for k, (src, dst) in enumerate(
                (
                    (nr_hbm.at[f], nr.at[f]),
                    (face(sol_hbm, f), sol.at[f]),
                    (face(dir_hbm, f), dirn.at[f]),
                    (prec_hbm.at[f], prec.at[f]),
                )
            )
        ]
        for f in range(2)
    ]
    for copy in loads[0] + loads[1]:
        copy.start()
    step = jnp.transpose(jnp.broadcast_to(rows[0:1, :], (W, W)))
    ratio = jnp.transpose(jnp.broadcast_to(rows[1:2, :], (W, W)))
    nprod_ref[...] = rows[2:3, :]
    outs = []

    def store(src, dst):
        copy = pltpu.make_async_copy(src, dst, osem.at[len(outs)])
        copy.start()
        outs.append(copy)

    for f in range(2):
        loads[f][0].wait()
        store(nr.at[f], face(nres_hbm, f))
        loads[f][1].wait()
        loads[f][2].wait()
        for b in range(FB):
            sol[f, :, cols(b)] += step * dirn[f, :, cols(b)]
        store(sol.at[f], face(nsol_hbm, f))
        loads[f][3].wait()
        for b in range(FB):
            prec[f, :, cols(b)] += ratio * dirn[f, :, cols(b)]
        store(prec.at[f], face(ndir_hbm, f))
    for copy in outs:
        copy.wait()


def shards(
    solution,
    residual,
    direction,
    residual_product,
    neighbor_slots,
    coupling,
    dirichlet_factor,
    face_block,
    neumann_factor,
    primal_block,
    primal_basis,
    coarse_matrix,
    coarse_block_inverse,
    coarse_pattern,
):
    hbm = pl.BlockSpec(memory_space=pl.ANY)
    vmem = pl.BlockSpec(memory_space=pltpu.VMEM)
    smem = pl.BlockSpec(memory_space=pltpu.SMEM)
    dma = pltpu.SemaphoreType.DMA
    big = jax.ShapeDtypeStruct((1, W, 2 * FACE), F32)
    pair = jax.ShapeDtypeStruct((2, W, FACE), F32)
    nr, prec, rows = pl.pallas_call(
        kernel,
        out_shape=(pair, pair, jax.ShapeDtypeStruct((8, W), F32)),
        in_specs=[hbm, hbm, vmem, smem, hbm, hbm, hbm, hbm, vmem, hbm, hbm, hbm, smem],
        out_specs=(hbm, hbm, vmem),
        scratch_shapes=[
            *[pltpu.VMEM((32, 2 * W, W), BF16)] * 3,
            *[pltpu.VMEM((32, W, W), BF16)] * 3,
            pltpu.VMEM((32, W, W), BF16),
            pltpu.VMEM((32, W, W), BF16),
            pltpu.VMEM((W, W), BF16),
            pltpu.VMEM((9, W, W), F32),
            pltpu.VMEM((W, W), F32),
            pltpu.VMEM((2, W, FACE), F32),
            pltpu.VMEM((4, W, FACE), F32),
            pltpu.VMEM((4, 2 * W, FACE), BF16),
            pltpu.VMEM((4, W, FACE), F32),
            pltpu.VMEM((4, W, 3 * W), F32),
            pltpu.VMEM((4, W, 3 * W), F32),
            pltpu.VMEM((2, W, FACE), F32),
            pltpu.VMEM((2, W, FACE), F32),
            pltpu.VMEM((2, W, FACE), F32),
            pltpu.VMEM((2, FB, W, W), F32),
            pltpu.VMEM((2, FB, W, W), F32),
            pltpu.VMEM((4, W + 8, W), F32),
            pltpu.VMEM((4, W + 8, W), F32),
            pltpu.VMEM((4, FB, W, 2 * W), BF16),
            pltpu.VMEM((2, W, W), F32),
            pltpu.VMEM((2, W, W), F32),
            pltpu.VMEM((4, W, W), F32),
            pltpu.VMEM((4, W, W), F32),
            pltpu.VMEM((2, W, W), F32),
            pltpu.VMEM((2, N_GRP, W, W), F32),
            pltpu.VMEM((2 * REACH + 1, N_GRP, W, W), F32),
            pltpu.VMEM((W, W), F32),
            pltpu.VMEM((2, W, W), F32),
            pltpu.VMEM((W, W), F32),
            pltpu.VMEM((W, W), F32),
            pltpu.VMEM((2, N_X * N_GRP, 8, W), F32),
            pltpu.VMEM((2, ROW, 8, W), F32),
            dma((15,)),
            dma((4,)),
            dma((4,)), dma((4,)),
            dma((2,)), dma((2,)),
            dma((4,)), dma((4,)),
            dma((2,)), dma((2,)),
            dma((4,)), dma((4,)),
            dma((2, FB)), dma((2, FB)),
            dma((2, 3)), dma((2, N_GRP)), dma((N_GRP, 4)), dma((2 * REACH + 1, N_GRP)),
            dma((2,)), dma((2,)),
            dma((2, N_X * N_GRP)), dma((2, N_X * N_GRP)),
            dma((2, ROW)), dma((2, ROW)),
        ],
        compiler_params=pltpu.CompilerParams(
            collective_id=0, has_side_effects=True, vmem_limit_bytes=60 * 1024 * 1024
        ),
        name="pcg_step",
    )(
        residual,
        direction,
        residual_product.reshape(1, W),
        neighbor_slots,
        coupling,
        dirichlet_factor,
        face_block,
        neumann_factor,
        primal_block,
        primal_basis,
        coarse_matrix,
        coarse_block_inverse,
        coarse_pattern,
    )
    nsol, nres, ndir, nprod = pl.pallas_call(
        finish,
        out_shape=(big, big, big, jax.ShapeDtypeStruct((1, W), F32)),
        in_specs=[hbm, hbm, hbm, hbm, vmem],
        out_specs=(hbm, hbm, hbm, vmem),
        scratch_shapes=[
            pltpu.VMEM((2, W, FACE), F32),
            pltpu.VMEM((2, W, FACE), F32),
            pltpu.VMEM((2, W, FACE), F32),
            pltpu.VMEM((2, W, FACE), F32),
            dma((2, 4)),
            dma((6,)),
        ],
        name="finish",
    )(solution, direction, nr, prec, rows)
    return nsol, nres, ndir, nprod.reshape(W)


def solution(mesh):
    both = ("sub", "grp")

    def split_first(rank):
        return P(both, *([None] * (rank - 1)))

    return jax.shard_map(
        shards,
        mesh=mesh,
        in_specs=(
            split_first(3), split_first(3), split_first(3), P(), split_first(2), split_first(4), split_first(4),
            split_first(4), split_first(4), split_first(2), split_first(3), split_first(4), split_first(3),
            split_first(2),
        ),
        out_specs=(split_first(3), split_first(3), split_first(3), P()),
        check_vma=False,
    )
```

```python
import functools

import jax
import jax.numpy as jnp
from jax import lax
from jax.experimental import pallas as pl
from jax.experimental.pallas import tpu as pltpu
from jax.sharding import PartitionSpec as P

F32 = jnp.float32
BF16 = jnp.bfloat16
MESH = pl.DeviceIdType.MESH

N_SUB = 32
N_GRP = 4
ROW = 8
N_X = N_SUB // ROW
W = 128
FB = 8
FACE = FB * W
REACH = 2


def split(x):
    hi = x.astype(BF16)
    lo = (x - hi.astype(F32)).astype(BF16)
    return hi, lo


def wide(x):
    return jnp.concatenate(split(x), 1)


def mm(x, w):
    return lax.dot_general(x, w, (((1,), (0,)), ((), ())), preferred_element_type=F32)


def mmt(x, w):
    return lax.dot_general(x, w, (((1,), (1,)), ((), ())), preferred_element_type=F32)


def mm3(x, w):
    xh, xl = split(x)
    wh, wl = split(w)
    return mm(jnp.concatenate([xh, xl], 1), jnp.concatenate([wh, wh], 0)) + mm(xh, wl)


def cols(b):
    return pl.ds(b * W, W)


def kernel(
    res_hbm, dir_hbm, rp_ref, slots, coup_hbm, diri_hbm, face_hbm, neum_hbm, pblk_ref, basis_hbm, cmat_hbm,
    cinv_hbm, patt,
    nr_hbm, prec_hbm, rows_ref,
    coup0, coup1, coup2, diri0, diri1, diri2, face, neum, basis, cmat, cinv, res,
    uf, uhl, yy, tt, ss, c2, nr, prec, nst, nf, bms, bmr, masks, crs, crr, cis, cir, ownc, steps, win, cors, corr_in,
    avec, z2, ar_p, ar_z,
    lsem, osem, dsend, drecv, nsend, nrecv, bsend, brecv, crsend, crrecv, cisend, cirecv, c2send, c2recv,
    wysend, wyrecv, wssend, wrecv, cosend, corecv, psend, precv, zsend, zrecv,
):
    i = lax.axis_index("sub")
    g = lax.axis_index("grp")
    row = i // ROW
    col = i % ROW

    def at_sub(k):
        return lax.rem(i + k + N_SUB, N_SUB)

    def at_grp(k):
        return lax.rem(g + k + N_GRP, N_GRP)

    def dev(s, t):
        return {"sub": s, "grp": t}

    neighbor = [dev(at_sub(-1), g), dev(at_sub(1), g), dev(i, at_grp(-1)), dev(i, at_grp(1))]
    y_peers = [dev(i, at_grp(k)) for k in range(1, N_GRP)]
    z_peers = [dev(row * ROW + lax.rem(col + k, ROW), g) for k in range(1, ROW)]
    plane = row * N_GRP + g
    many_plane = N_X * N_GRP

    def in_plane(k):
        other = lax.rem(plane + k, many_plane)
        return dev(other // N_GRP * ROW + col, lax.rem(other, N_GRP))

    p_peers = [in_plane(k) for k in range(1, many_plane)]
    reach = [k for k in range(-REACH, REACH + 1) if k != 0]
    s_peers = [dev(at_sub(k), g) for k in reach]
    odd = lax.rem(i, 2)
    far = [dev(at_sub(REACH), g), dev(at_sub(-REACH), g)]
    partner = dev(i + 1 - 2 * odd, g)

    local = []

    def load(src, dst):
        copy = pltpu.make_async_copy(src, dst, lsem.at[len(local)])
        copy.start()
        local.append(copy)
        return copy

    coup = (coup0, coup1, coup2)
    diri = (diri0, diri1, diri2)
    many = 4 * FB
    l_basis = load(basis_hbm.at[0], basis)
    l_dir = [load(dir_hbm.at[0, :, pl.ds(f * FACE, FACE)], uf.at[2 * f + 1]) for f in (1, 0)]
    l_face = load(face_hbm.at[0], face)
    l_interior = []
    for q in range(3):
        if q == 1:
            l_neum = load(neum_hbm.at[0], neum)
        l_interior.append(
            (
                load(coup_hbm.at[0, pl.ds(q * many, many)], coup[q]),
                load(diri_hbm.at[0, pl.ds(q * many, many)], diri[q]),
            )
        )
    l_res = [load(res_hbm.at[0, :, pl.ds(f * FACE, FACE)], res.at[f]) for f in range(2)]
    l_cinv = load(cinv_hbm.at[0], cinv)
    l_cmat = load(cmat_hbm.at[0], cmat)

    barrier = pltpu.get_barrier_semaphore()
    everyone = p_peers + z_peers + s_peers
    for peer in everyone:
        pl.semaphore_signal(barrier, inc=1, device_id=peer, device_id_type=MESH)
    pl.semaphore_wait(barrier, len(everyone))

    sent = []

    def send(src, dst, send_sem, recv_sem, peer):
        copy = pltpu.make_async_remote_copy(
            src_ref=src, dst_ref=dst, send_sem=send_sem, recv_sem=recv_sem, device_id=peer, device_id_type=MESH
        )
        copy.start()
        sent.append(copy)

    def arrived(ref, send_sem, recv_sem):
        pltpu.make_async_remote_copy(
            src_ref=ref, dst_ref=ref, send_sem=send_sem, recv_sem=recv_sem, device_id=neighbor[0], device_id_type=MESH
        ).wait_recv()

    chunks = ((0, 4), (4, 6), (6, FB))

    def chunk(h):
        return pl.ds(chunks[h][0] * W, (chunks[h][1] - chunks[h][0]) * W)

    for h, (start, stop) in enumerate(chunks):
        send(
            dir_hbm.at[0, :, pl.ds(FACE + start * W, (stop - start) * W)], uf.at[2, :, chunk(h)],
            dsend.at[h], drecv.at[h], neighbor[3],
        )
    half = FACE // 2
    for h in range(2):
        part = pl.ds(h * half, half)
        send(dir_hbm.at[0, :, part], uf.at[0, :, part], dsend.at[3 + h], drecv.at[3 + h], neighbor[1])

    l_basis.wait()
    pb_row = pblk_ref[...].astype(F32)
    basis_t = jnp.transpose(basis[...].astype(F32))
    for d in range(4):
        bms[d, 0:W, :] = basis_t
        bms[d, W : W + 8, :] = jnp.broadcast_to(pb_row - (slots[0, d] * FB).astype(F32), (8, W))

    def send_basis(d):
        send(bms.at[d], bmr.at[d ^ 1], bsend.at[d], brecv.at[d ^ 1], neighbor[d])

    def basis_arrived(d):
        arrived(bmr.at[d], bsend.at[d], brecv.at[d])
        nb_masks(d)

    for d in (2, 0):
        send_basis(d)
    def own_masks(d, carry):
        for b in range(FB):
            number = (slots[0, d] * FB + b).astype(F32)
            masks[d, b, :, 0:W] = jnp.where(pb_row == number, bms[0, 0:W, :], 0.0).astype(BF16)
        return carry

    lax.fori_loop(0, 4, own_masks, 0)

    def nb_masks(d):
        rel = bmr[d, W : W + 1, :]
        for b in range(FB):
            masks[d, b, :, W : 2 * W] = jnp.where(rel == float(b), bmr[d, 0:W, :], 0.0).astype(BF16)

    def coarse_pair(read, d):
        sums = [None, None]
        for b in range(FB):
            both = masks[d, b]
            part = mm(wide(read(b)), jnp.concatenate([both, both], 0))
            sums[b % 2] = part if sums[b % 2] is None else sums[b % 2] + part
        return sums[0] + sums[1]

    l_dir[0].wait()
    l_face.wait()
    for copy in l_interior[0]:
        copy.wait()

    def chain(jobs):
        first = []
        for (hi, lo), n in jobs:
            m = coup[n[0]][n[1]]
            first.append(wide(mm(jnp.concatenate([hi, lo], 1), jnp.concatenate([m, m], 0))))
        second = []
        for x, (_, n) in zip(first, jobs):
            m = diri[n[0]][n[1]]
            second.append(wide(mm(x, jnp.concatenate([m, m], 0))))
        third = []
        for x, (_, n) in zip(second, jobs):
            m = diri[n[0]][n[1]]
            third.append(wide(mmt(x, jnp.concatenate([m, m], 1))))
        out = []
        for x, (_, n) in zip(third, jobs):
            m = coup[n[0]][n[1]]
            out.append(mmt(x, jnp.concatenate([m, m], 1)))
        return out

    def interior(jobs, size=9):
        out = []
        for k in range(0, len(jobs), size):
            out += chain(jobs[k : k + size])
        return out

    def pair_of(d, b, e, c):
        hi = jnp.concatenate([uhl[d, 0:W, cols(b)], uhl[e, 0:W, cols(c)]], 1)
        lo = jnp.concatenate([uhl[d, W : 2 * W, cols(b)], uhl[e, W : 2 * W, cols(c)]], 1)
        return hi, lo

    def face_term(d, blocks):
        base = slots[0, d] * FB
        for b in blocks:
            hi, lo = split(uf[d, :, cols(b)])
            uhl[d, 0:W, cols(b)] = hi
            uhl[d, W : 2 * W, cols(b)] = lo
            m = face[base + b]
            yy[d, :, cols(b)] = mm(jnp.concatenate([hi, lo], 1), jnp.concatenate([m, m], 0))

    def within_jobs(d, pairs):
        base = slots[0, d] * FB
        return [(pair_of(d, b, d, b + q + 1), (q, base + b)) for q, b in pairs]

    def within_sink(d, pairs, outs):
        for (q, b), out in zip(pairs, outs):
            yy[d, :, cols(b)] += out[:, :W]
            yy[d, :, cols(b + q + 1)] += out[:, W:]

    def within(d, pairs):
        within_sink(d, pairs, interior(within_jobs(d, pairs)))

    inside = [(q, b) for q in range(3) for b in range(FB - 1 - q)]
    early, middle, late = [[(q, b) for q, b in inside if start <= b + q + 1 < stop] for start, stop in chunks]
    across = [(q, b) for q in range(3) for b in range(FB - 1 - q, FB)]

    def direction_of(slot):
        where = jnp.int32(0)
        for d in range(1, 4):
            where = jnp.where(slots[0, d] == slot, jnp.int32(d), where)
        return where

    def straddling_jobs(places):
        jobs = []
        for p in places:
            slot = lax.rem(slots[0, 2] + 1 + p, 4)
            this = direction_of(slot)
            after = direction_of(lax.rem(slot + 1, 4))
            for q, b in across:
                jobs.append((pair_of(this, b, after, b + q + 1 - FB), (q, slot * FB + b)))
        return jobs

    def straddling_sink(places, outs):
        sinks = [(p, b - FB + 3, b + q + 1 - FB) for p in places for q, b in across]
        heads, tails = {}, {}
        for (p, h, m), out in zip(sinks, outs):
            heads[p, h] = heads[p, h] + out[:, :W] if (p, h) in heads else out[:, :W]
            tails[p, m] = tails[p, m] + out[:, W:] if (p, m) in tails else out[:, W:]
        for (p, m), value in heads.items():
            tt[p, :, cols(m)] = value
        for (p, m), value in tails.items():
            ss[p, :, cols(m)] = value

    def return_piece(f, k):
        piece = cols(k)
        send(
            yy.at[2 * f, :, piece], c2.at[f, :, piece], c2send.at[f, k], c2recv.at[f, k], neighbor[2 * f]
        )

    def returned(f, blocks):
        for k in blocks:
            piece = cols(k)
            arrived(c2.at[f, :, piece], c2send.at[f, k], c2recv.at[f, k])

    def first_step(v, value):
        ownc[v] = value
        steps[v, g] = mm3(value, cinv[...])
        for k, peer in enumerate(y_peers):
            send(steps.at[v, g], steps.at[v, g], wysend.at[v, k], wyrecv.at[v, g], peer)

    def forward(k):
        piece = at_grp(k)
        if k > 0:
            for v in range(2):
                arrived(steps.at[v, piece], wysend.at[v, 0], wyrecv.at[v, piece])
        win[REACH, piece] = 0.5 * (steps[0, piece] - avec[...] * steps[1, piece])
        for n, (place, peer) in enumerate(zip((0, 2 * REACH, 1 + 2 * odd), far + [partner])):
            send(win.at[REACH, piece], win.at[place, piece], wssend.at[k, n], wrecv.at[place, piece], peer)

    def relay(k):
        piece = at_grp(k)
        place, there = 2 * REACH * (1 - odd), 3 - 2 * odd
        arrived(win.at[place, piece], wssend.at[0, 0], wrecv.at[place, piece])
        send(win.at[place, piece], win.at[there, piece], wssend.at[k, 3], wrecv.at[there, piece], partner)

    def complete():
        for k in range(N_GRP):
            piece = at_grp(k)
            for place in (2 * REACH * odd, 1, 3):
                arrived(win.at[place, piece], wssend.at[0, 0], wrecv.at[place, piece])

    face_term(3, range(FB))
    within(3, [(q, b) for q, b in inside if q == 0])
    for copy in l_interior[1]:
        copy.wait()
    within(3, [(q, b) for q, b in inside if q == 1])
    for copy in l_interior[2]:
        copy.wait()
    within(3, [(q, b) for q, b in inside if q == 2])
    l_neum.wait()
    for f in (1, 0):
        start = slots[0, 2 * f] * FB

        def to_f32(b, carry, f=f, start=start):
            nst[f, b] = neum[start + b].astype(F32)
            return carry

        lax.fori_loop(0, FB, to_f32, 0)
        send(nst.at[f], nf.at[f], nsend.at[f], nrecv.at[f], neighbor[2 * f])

    basis_arrived(3)
    basis_arrived(1)
    for copy in l_res:
        copy.wait()

    pairs = [coarse_pair(lambda b, f=f: res[f, :, cols(b)], 2 * f + 1) for f in range(2)]
    ownc[0] = pairs[0][:, :W] + pairs[1][:, :W]
    for f in range(2):
        crs[f] = pairs[f][:, W:]
    for f in range(2):
        send(crs.at[f], crr.at[f], crsend.at[f], crrecv.at[f], neighbor[2 * f + 1])
    send_basis(3)
    send_basis(1)

    l_dir[1].wait()
    face_term(1, range(FB))
    within(1, inside)

    arrived(uf.at[0, :, pl.ds(0, half)], dsend.at[3], drecv.at[3])
    face_term(0, range(FB // 2))
    within(0, early)
    arrived(uf.at[2, :, chunk(0)], dsend.at[0], drecv.at[0])
    face_term(2, range(*chunks[0]))
    within(2, early)
    arrived(uf.at[0, :, pl.ds(half, half)], dsend.at[4], drecv.at[4])
    face_term(0, range(FB // 2, FB))
    within(0, middle + late)
    straddling_sink((0, 1, 2), interior(straddling_jobs((0, 1, 2))))
    place = lax.rem(slots[0, 0] - slots[0, 2] + 7, 4)
    for m in range(3):
        yy[0, :, cols(FB - 3 + m)] += tt[place, :, cols(m)]
    for k in range(3, FB):
        return_piece(0, k)
    basis_arrived(0)
    arrived(uf.at[2, :, chunk(1)], dsend.at[1], drecv.at[1])
    face_term(2, range(*chunks[1]))
    within(2, middle)
    for m in range(3):
        yy[2, :, cols(m)] += ss[2, :, cols(m)]
    return_piece(1, 0)
    return_piece(1, 1)
    arrived(uf.at[2, :, chunk(2)], dsend.at[2], drecv.at[2])
    face_term(2, range(*chunks[2]))
    outs = interior(within_jobs(2, late) + straddling_jobs((3,)), 6)
    within_sink(2, late, outs[: len(late)])
    straddling_sink((3,), outs[len(late) :])
    for d in range(4):
        place = lax.rem(slots[0, d] - slots[0, 2] + 7, 4)
        before = lax.rem(slots[0, d] - slots[0, 2] + 6, 4)
        for m in range(3):
            if d != 2:
                yy[d, :, cols(m)] += ss[before, :, cols(m)]
            if d != 0:
                yy[d, :, cols(FB - 3 + m)] += tt[place, :, cols(m)]

    def folded(x):
        return jnp.sum(jnp.transpose(x).reshape(W // 8, 8, W), axis=0)

    stages = (
        (ar_p, psend, precv, many_plane, plane, p_peers),
        (ar_z, zsend, zrecv, ROW, col, z_peers),
    )

    def stage_send(which, stage, value):
        buf, ssem, rsem, count, me, peers = stages[stage]
        buf[which, me] = value
        for k, peer in enumerate(peers):
            send(buf.at[which, me], buf.at[which, me], ssem.at[which, k], rsem.at[which, me], peer)

    def stage_wait(which, stage):
        buf, ssem, rsem, count, me, peers = stages[stage]
        for k in range(1, count):
            other = lax.rem(me + k, count)
            arrived(buf.at[which, other], ssem.at[which, 0], rsem.at[which, other])
        total = buf[which, 0]
        for k in range(1, count):
            total = total + buf[which, k]
        return total

    def curve(d, acc):
        for b in range(FB):
            acc = acc + uf[d, :, cols(b)] * yy[d, :, cols(b)]
        return acc

    stage_send(0, 0, folded(lax.fori_loop(0, 4, curve, jnp.zeros((W, W), F32))))

    basis_arrived(2)

    for first in (2, 0):
        pairs = [coarse_pair(lambda b, d=d: yy[d, :, cols(b)], d) for d in (first, first + 1)]
        for d, pair in zip((first, first + 1), pairs):
            cis[d] = pair[:, W:]
            send(cis.at[d], cir.at[d ^ 1], cisend.at[d], cirecv.at[d ^ 1], neighbor[d])
        both = pairs[0][:, :W] + pairs[1][:, :W]
        ownc[1] = both if first == 2 else ownc[1] + both

    for f in range(2):
        arrived(crr.at[f], crsend.at[f], crrecv.at[f])
    l_cinv.wait()
    first_step(0, ownc[0] + (crr[0] + crr[1]))
    stage_send(0, 1, stage_wait(0, 0))
    for k in range(3):
        return_piece(0, k)
    for k in range(2, 3):
        return_piece(1, k)
    for d in range(4):
        arrived(cir.at[d], cisend.at[d], cirecv.at[d])
    first_step(1, ownc[1] + ((cir[0] + cir[1]) + (cir[2] + cir[3])))
    for k in range(3, FB):
        return_piece(1, k)
    rp_row = rp_ref[...]
    curvature = jnp.sum(stage_wait(0, 1), axis=0, keepdims=True)
    step_row = rp_row / curvature
    avec[...] = jnp.transpose(jnp.broadcast_to(step_row, (W, W)))
    forward(0)
    for k in range(1, N_GRP):
        forward(k)
    relay(0)

    outs = []

    def store(src, dst):
        copy = pltpu.make_async_copy(src, dst, osem.at[len(outs)])
        copy.start()
        outs.append(copy)

    z2[...] = jnp.zeros_like(z2)

    def own_face(f, blocks):
        a = avec[...]
        base = slots[0, 2 * f + 1] * FB
        acc = z2[...]
        for b in blocks:
            new = res[f, :, cols(b)] - a * (yy[2 * f + 1, :, cols(b)] + c2[f, :, cols(b)])
            nr[f, :, cols(b)] = new
            mine = neum[base + b]
            theirs = nf[f, b].astype(BF16)
            both = jnp.concatenate([mine, theirs], 1)
            z = mm(wide(0.5 * new), jnp.concatenate([both, both], 0))
            acc = acc + (z[:, :W] * z[:, :W] + z[:, W:] * z[:, W:])
            lhs = jnp.concatenate([wide(z[:, :W]), wide(z[:, W:])], 1)
            prec[f, :, cols(b)] = mmt(lhs, jnp.concatenate([mine, mine, theirs, theirs], 1))
        z2[...] = acc

    returned(0, range(FB))
    arrived(nf.at[0], nsend.at[0], nrecv.at[0])
    own_face(0, range(FB))
    relay(1)
    arrived(nf.at[1], nsend.at[1], nrecv.at[1])
    returned(1, range(4))
    own_face(1, range(4))
    relay(2)
    returned(1, range(4, FB))
    own_face(1, range(4, FB))
    for f in range(2):
        store(nr.at[f], nr_hbm.at[f])

    relay(3)
    complete()
    l_cmat.wait()
    adjacent = None
    for k in range(9):
        entry = patt[0, k]
        place = jnp.minimum(lax.rem(entry // N_GRP - i + REACH + N_SUB, N_SUB), 2 * REACH)
        part = mm3(win[place, lax.rem(entry, N_GRP)], cmat[k])
        adjacent = part if adjacent is None else adjacent + part
    coarse_res = 0.5 * (ownc[0] - avec[...] * ownc[1])
    corr = win[REACH, g] + mm3(coarse_res - adjacent, cinv[...])
    cors[...] = corr
    stage_send(1, 0, folded(z2[...] + corr * coarse_res))
    for f in (1, 0):
        send(cors, corr_in.at[f], cosend.at[f], corecv.at[f], neighbor[2 * f])
    stage_send(1, 1, stage_wait(1, 0))
    for f in range(2):
        arrived(corr_in.at[f], cosend.at[f], corecv.at[f])

    def spread_back(f, carry):
        lhs = jnp.concatenate([wide(cors[...]), wide(corr_in[f])], 1)
        for b in range(FB):
            own = masks[2 * f + 1, b, :, 0:W]
            other = masks[2 * f + 1, b, :, W : 2 * W]
            back = mmt(lhs, jnp.concatenate([own, own, other, other], 1))
            prec[f, :, cols(b)] = 0.5 * (prec[f, :, cols(b)] + back)
        return carry

    lax.fori_loop(0, 2, spread_back, 0)
    for f in range(2):
        store(prec.at[f], prec_hbm.at[f])

    product = jnp.sum(stage_wait(1, 1), axis=0, keepdims=True)
    rows_ref[0:1, :] = step_row
    rows_ref[1:2, :] = product / rp_row
    rows_ref[2:3, :] = product
    for copy in sent:
        copy.wait_send()
    for copy in outs:
        copy.wait()


def finish(
    sol_hbm, dir_hbm, nr_hbm, prec_hbm, rows, nsol_hbm, nres_hbm, ndir_hbm, nprod_ref, sol, dirn, nr, prec, lsem, osem
):
    def face(ref, f):
        return ref.at[0, :, pl.ds(f * FACE, FACE)]

    loads = [
        [
            pltpu.make_async_copy(src, dst, lsem.at[f, k])
            for k, (src, dst) in enumerate(
                (
                    (nr_hbm.at[f], nr.at[f]),
                    (face(sol_hbm, f), sol.at[f]),
                    (face(dir_hbm, f), dirn.at[f]),
                    (prec_hbm.at[f], prec.at[f]),
                )
            )
        ]
        for f in range(2)
    ]
    for copy in loads[0] + loads[1]:
        copy.start()
    step = jnp.transpose(jnp.broadcast_to(rows[0:1, :], (W, W)))
    ratio = jnp.transpose(jnp.broadcast_to(rows[1:2, :], (W, W)))
    nprod_ref[...] = rows[2:3, :]
    outs = []

    def store(src, dst):
        copy = pltpu.make_async_copy(src, dst, osem.at[len(outs)])
        copy.start()
        outs.append(copy)

    for f in range(2):
        loads[f][0].wait()
        store(nr.at[f], face(nres_hbm, f))
        loads[f][1].wait()
        loads[f][2].wait()
        for b in range(FB):
            sol[f, :, cols(b)] += step * dirn[f, :, cols(b)]
        store(sol.at[f], face(nsol_hbm, f))
        loads[f][3].wait()
        for b in range(FB):
            prec[f, :, cols(b)] += ratio * dirn[f, :, cols(b)]
        store(prec.at[f], face(ndir_hbm, f))
    for copy in outs:
        copy.wait()


def shards(
    solution,
    residual,
    direction,
    residual_product,
    neighbor_slots,
    coupling,
    dirichlet_factor,
    face_block,
    neumann_factor,
    primal_block,
    primal_basis,
    coarse_matrix,
    coarse_block_inverse,
    coarse_pattern,
):
    hbm = pl.BlockSpec(memory_space=pl.ANY)
    vmem = pl.BlockSpec(memory_space=pltpu.VMEM)
    smem = pl.BlockSpec(memory_space=pltpu.SMEM)
    dma = pltpu.SemaphoreType.DMA
    big = jax.ShapeDtypeStruct((1, W, 2 * FACE), F32)
    pair = jax.ShapeDtypeStruct((2, W, FACE), F32)
    nr, prec, rows = pl.pallas_call(
        kernel,
        out_shape=(pair, pair, jax.ShapeDtypeStruct((8, W), F32)),
        in_specs=[hbm, hbm, vmem, smem, hbm, hbm, hbm, hbm, vmem, hbm, hbm, hbm, smem],
        out_specs=(hbm, hbm, vmem),
        scratch_shapes=[
            *[pltpu.VMEM((32, 2 * W, W), BF16)] * 3,
            *[pltpu.VMEM((32, W, W), BF16)] * 3,
            pltpu.VMEM((32, W, W), BF16),
            pltpu.VMEM((32, W, W), BF16),
            pltpu.VMEM((W, W), BF16),
            pltpu.VMEM((9, W, W), F32),
            pltpu.VMEM((W, W), F32),
            pltpu.VMEM((2, W, FACE), F32),
            pltpu.VMEM((4, W, FACE), F32),
            pltpu.VMEM((4, 2 * W, FACE), BF16),
            pltpu.VMEM((4, W, FACE), F32),
            pltpu.VMEM((4, W, 3 * W), F32),
            pltpu.VMEM((4, W, 3 * W), F32),
            pltpu.VMEM((2, W, FACE), F32),
            pltpu.VMEM((2, W, FACE), F32),
            pltpu.VMEM((2, W, FACE), F32),
            pltpu.VMEM((2, FB, W, W), F32),
            pltpu.VMEM((2, FB, W, W), F32),
            pltpu.VMEM((4, W + 8, W), F32),
            pltpu.VMEM((4, W + 8, W), F32),
            pltpu.VMEM((4, FB, W, 2 * W), BF16),
            pltpu.VMEM((2, W, W), F32),
            pltpu.VMEM((2, W, W), F32),
            pltpu.VMEM((4, W, W), F32),
            pltpu.VMEM((4, W, W), F32),
            pltpu.VMEM((2, W, W), F32),
            pltpu.VMEM((2, N_GRP, W, W), F32),
            pltpu.VMEM((2 * REACH + 1, N_GRP, W, W), F32),
            pltpu.VMEM((W, W), F32),
            pltpu.VMEM((2, W, W), F32),
            pltpu.VMEM((W, W), F32),
            pltpu.VMEM((W, W), F32),
            pltpu.VMEM((2, N_X * N_GRP, 8, W), F32),
            pltpu.VMEM((2, ROW, 8, W), F32),
            dma((15,)),
            dma((4,)),
            dma((5,)), dma((5,)),
            dma((2,)), dma((2,)),
            dma((4,)), dma((4,)),
            dma((2,)), dma((2,)),
            dma((4,)), dma((4,)),
            dma((2, FB)), dma((2, FB)),
            dma((2, 3)), dma((2, N_GRP)), dma((N_GRP, 4)), dma((2 * REACH + 1, N_GRP)),
            dma((2,)), dma((2,)),
            dma((2, N_X * N_GRP)), dma((2, N_X * N_GRP)),
            dma((2, ROW)), dma((2, ROW)),
        ],
        compiler_params=pltpu.CompilerParams(
            collective_id=0, has_side_effects=True, vmem_limit_bytes=60 * 1024 * 1024
        ),
        name="pcg_step",
    )(
        residual,
        direction,
        residual_product.reshape(1, W),
        neighbor_slots,
        coupling,
        dirichlet_factor,
        face_block,
        neumann_factor,
        primal_block,
        primal_basis,
        coarse_matrix,
        coarse_block_inverse,
        coarse_pattern,
    )
    nsol, nres, ndir, nprod = pl.pallas_call(
        finish,
        out_shape=(big, big, big, jax.ShapeDtypeStruct((1, W), F32)),
        in_specs=[hbm, hbm, hbm, hbm, vmem],
        out_specs=(hbm, hbm, hbm, vmem),
        scratch_shapes=[
            pltpu.VMEM((2, W, FACE), F32),
            pltpu.VMEM((2, W, FACE), F32),
            pltpu.VMEM((2, W, FACE), F32),
            pltpu.VMEM((2, W, FACE), F32),
            dma((2, 4)),
            dma((6,)),
        ],
        name="finish",
    )(solution, direction, nr, prec, rows)
    return nsol, nres, ndir, nprod.reshape(W)


def solution(mesh):
    both = ("sub", "grp")

    def split_first(rank):
        return P(both, *([None] * (rank - 1)))

    return jax.shard_map(
        shards,
        mesh=mesh,
        in_specs=(
            split_first(3), split_first(3), split_first(3), P(), split_first(2), split_first(4), split_first(4),
            split_first(4), split_first(4), split_first(2), split_first(3), split_first(4), split_first(3),
            split_first(2),
        ),
        out_specs=(split_first(3), split_first(3), split_first(3), P()),
        check_vma=False,
    )
```
